8 devices in a mesh: dp: 1 (over z), tp: 2 (over y), cp: 4 (over x, core).
Axes of the slice: x: 2, y: 2, z: 1, core: 2. Of those that a mesh axis runs over, the one named last changes fastest.
Arguments:
- x_tokens: bfloat16 [256, 3072], P(('dp', 'cp', 'tp'))
- w_q: bfloat16 [3072, 16, 256], P(None, 'tp')
- w_k: bfloat16 [3072, 16, 256], P(None, 'tp')
- w_v: bfloat16 [3072, 16, 256], P(None, 'tp')
- w_o: bfloat16 [16, 256, 3072], P('tp')
Outputs:
- output: bfloat16 [256, 3072], P(('dp', 'cp', 'tp'))
All inputs are finite; a program needn't handle non-finite values.
Results may differ from the reference program's by a relative error of at most 0.00540522.
Values are sent between devices in bfloat16 or wider.
A program may use at most 1 GiB of HBM per device.

```python
import jax
import jax.numpy as jnp
from jax import lax

SEQ_LEN = 256
CP_SIZE = 4
D_MODEL = 3072
NUM_HEADS = 16
HEAD_DIM = 256


def setup_inputs(seed: int = 0, part: int = 0) -> dict:
    root_key = jax.random.key(seed)
    x_key = jax.random.fold_in(jax.random.fold_in(root_key, 1), part)
    q_key, k_key, v_key, o_key = jax.random.split(jax.random.fold_in(root_key, 2), 4)
    in_scale = D_MODEL ** -0.5
    out_scale = (NUM_HEADS * HEAD_DIM) ** -0.5
    head_shape = (D_MODEL, NUM_HEADS, HEAD_DIM)
    x_tokens = jax.random.normal(x_key, (SEQ_LEN, D_MODEL), jnp.float32)
    w_q = jax.random.normal(q_key, head_shape, jnp.float32) * (2.5 * in_scale)
    w_k = jax.random.normal(k_key, head_shape, jnp.float32) * in_scale
    w_v = jax.random.normal(v_key, head_shape, jnp.float32) * in_scale
    w_o = jax.random.normal(o_key, (NUM_HEADS, HEAD_DIM, D_MODEL), jnp.float32) * out_scale
    return {'x_tokens': x_tokens.astype(jnp.bfloat16), 'w_q': w_q.astype(jnp.bfloat16), 'w_k': w_k.astype(jnp.bfloat16), 'w_v': w_v.astype(jnp.bfloat16), 'w_o': w_o.astype(jnp.bfloat16)}


def token_positions():
    shard_len = SEQ_LEN // CP_SIZE
    block_len = shard_len // 2
    token_idx = jnp.arange(SEQ_LEN, dtype=jnp.int32)
    owner_shard = token_idx // shard_len
    within = token_idx % shard_len
    nat_block = jnp.where(within < block_len, owner_shard, 2 * CP_SIZE - 1 - owner_shard)
    return nat_block * block_len + within % block_len


def reference(x_tokens, w_q, w_k, w_v, w_o):
    def project(weight):
        flat = jnp.dot(x_tokens, weight.reshape(D_MODEL, NUM_HEADS * HEAD_DIM), preferred_element_type=jnp.float32)
        return flat.astype(jnp.bfloat16).reshape(SEQ_LEN, NUM_HEADS, HEAD_DIM).transpose(1, 0, 2)

    q_heads = project(w_q)
    k_heads = project(w_k)
    v_heads = project(w_v)
    positions = token_positions()
    n_blocks = 2 * CP_SIZE
    block_len = SEQ_LEN // n_blocks
    inv_sqrt = HEAD_DIM ** -0.5

    def one_head(head_args):
        q_head, k_head, v_head = head_args

        def one_block(block_args):
            q_blk, q_pos = block_args
            scores = jnp.dot(q_blk, k_head.T, preferred_element_type=jnp.float32) * inv_sqrt
            causal_mask = positions[None, :] <= q_pos[:, None]
            scores = jnp.where(causal_mask, scores, -1e30)
            weights = jnp.exp(scores - scores.max(axis=-1, keepdims=True))
            row_total = weights.sum(axis=-1, keepdims=True)
            block_out = jnp.dot(weights.astype(jnp.bfloat16), v_head, preferred_element_type=jnp.float32) / row_total
            return block_out.astype(jnp.bfloat16)

        head_blocks = lax.map(one_block, (q_head.reshape(n_blocks, block_len, HEAD_DIM), positions.reshape(n_blocks, block_len)))
        return head_blocks.reshape(SEQ_LEN, HEAD_DIM)

    attn_heads = lax.map(one_head, (q_heads, k_heads, v_heads))
    attn_flat = attn_heads.transpose(1, 0, 2).reshape(SEQ_LEN, NUM_HEADS * HEAD_DIM)
    y_full = jnp.dot(attn_flat, w_o.reshape(NUM_HEADS * HEAD_DIM, D_MODEL), preferred_element_type=jnp.float32)
    return y_full.astype(jnp.bfloat16)
```

```python
import functools

import jax
import jax.numpy as jnp
from jax import lax
from jax.experimental import pallas as pl
from jax.experimental.pallas import tpu as pltpu
from jax.sharding import PartitionSpec as P

MESH = pl.DeviceIdType.MESH
BF16 = jnp.bfloat16
F32 = jnp.float32

ROWS = 32
SEQ = 256
D = 3072
E = 256
HC = 4
KB = 512
NK = D // KB
NB = 256
NN = D // NB
NEG = -1e30
OWN_Y, OWN_X, OWN_C, FWD, Y_C, X_C, G_C = range(7)


def kernel(x_hbm, wq_hbm, wk_hbm, wv_hbm, wo_hbm, out_ref,
           xg, raw, wd, wo, qkv, oall, oown, orecv, yown, ysend, yrecv,
           x_sem, w_sem, wo_sem, xs_sem, xr_sem, os_sem, or_sem, ys_sem, yr_sem):
    t = lax.axis_index("tp")
    cp = lax.axis_index("cp")
    xx = cp // 2
    c = cp % 2
    cx = (cp + 2) % 4
    to_y = {"tp": 1 - t}
    to_x = {"cp": cx}
    to_c = {"cp": cp + 1 - 2 * c}

    def block(tt, pp):
        return pp + tt * (7 - 2 * pp)

    own = block(t, cp)
    b_y = block(1 - t, cp)
    b_x = block(t, cx)
    b_g = block(1 - t, cx)

    def x_rows(b, k):
        return xg.at[pl.ds(pl.multiple_of(b * ROWS, ROWS), ROWS), pl.ds(pl.multiple_of(k * KB, KB), KB)]

    x_copy = pltpu.make_async_copy(x_hbm, xg.at[pl.ds(pl.multiple_of(own * ROWS, ROWS), ROWS), :], x_sem)
    x_copy.start()

    def w_copy(m, k, half):
        src = (wq_hbm, wk_hbm, wv_hbm)[m]
        return pltpu.make_async_copy(src.at[k, half, :, :, c], raw.at[m, k, :, :, pl.ds(4 * half, 4)], w_sem.at[m, k, half])

    for k in range(NK):
        for m in range(3):
            for half in range(2):
                w_copy(m, k, half).start()

    def wo_copy():
        return pltpu.make_async_copy(wo_hbm, wo, wo_sem)

    wo_copy().start()

    barrier = pltpu.get_barrier_semaphore()
    for peer in (to_y, to_x, to_c):
        pl.semaphore_signal(barrier, inc=1, device_id=peer, device_id_type=MESH)
    pl.semaphore_wait(barrier, 3)

    def send(kind, k, b, peer):
        return pltpu.make_async_remote_copy(
            src_ref=x_rows(b, k), dst_ref=x_rows(b, k), send_sem=xs_sem.at[kind, k], recv_sem=xr_sem.at[kind, k],
            device_id=peer, device_id_type=MESH)

    x_copy.wait()
    for k in range(NK):
        send(OWN_Y, k, own, to_y).start()
        send(OWN_X, k, own, to_x).start()
    for k in range(NK):
        send(OWN_C, k, own, to_c).start()

    def handle_direct(k):
        send(OWN_Y, k, b_y, to_y).wait_recv()
        if isinstance(k, int):
            even = k % 2 == 0
        send(Y_C, k, b_y, to_c).start()
        if even:
            send(FWD, k, b_y, to_x).start()
        send(OWN_X, k, b_x, to_x).wait_recv()
        send(X_C, k, b_x, to_c).start()
        if not even:
            send(FWD, k, b_x, to_y).start()

    def handle_diag(k):
        send(FWD, k, b_g, to_x).wait_recv()
        send(G_C, k, b_g, to_c).start()

    def deint(m, k):
        for half in range(2):
            w_copy(m, k, half).wait()
        for j in range(2):
            for q in range(4):
                v = jnp.swapaxes(raw[m, k, pl.ds(q * 64, 64), j], 0, 1)
                for half in range(2):
                    for h in range(HC):
                        wd[m * HC + h, pl.ds(k * KB + half * 256 + q * 64, 64), pl.ds(j * 128, 128)] = v[half * 4 + h]

    for k in range(NK):
        for m in range(3):
            deint(m, k)
        if k >= 1:
            handle_direct(k - 1)
        if k >= 3:
            handle_diag(k - 3)
    handle_direct(NK - 1)
    for k in range(NK - 3, NK):
        handle_diag(k)
    p_own = block(t, cp + 1 - 2 * c)
    p_y = block(1 - t, cp + 1 - 2 * c)
    p_cp = (cp + 1 - 2 * c + 2) % 4
    p_x = block(t, p_cp)
    p_g = block(1 - t, p_cp)
    for k in range(NK):
        send(OWN_C, k, p_own, to_c).wait_recv()
        send(Y_C, k, p_y, to_c).wait_recv()
        send(X_C, k, p_x, to_c).wait_recv()
        send(G_C, k, p_g, to_c).wait_recv()

    def project(i, _):
        qkv[i] = jnp.dot(xg[...], wd[i], preferred_element_type=F32).astype(BF16)
        return 0

    lax.fori_loop(0, 3 * HC, project, 0)

    lo0 = pl.multiple_of(xx * 64, 64)
    hi0 = pl.multiple_of(192 - xx * 64, 64)

    def attend(h, start, n_keys):
        q = qkv[h, pl.ds(start, 64), :]
        kk = qkv[HC + h, :n_keys, :]
        vv = qkv[2 * HC + h, :n_keys, :]
        s = lax.dot_general(q, kk, (((1,), (1,)), ((), ())), preferred_element_type=F32) * (E ** -0.5)
        rows = start + lax.broadcasted_iota(jnp.int32, (64, n_keys), 0)
        cols = lax.broadcasted_iota(jnp.int32, (64, n_keys), 1)
        s = jnp.where(cols <= rows, s, NEG)
        m = jnp.max(s, axis=-1, keepdims=True)
        p = jnp.exp(s - m)
        l = jnp.sum(p, axis=-1, keepdims=True)
        o = jnp.dot(p.astype(BF16), vv, preferred_element_type=F32)
        return (o / l).astype(BF16)

    def o_copy(h, part):
        src = 2 * part + (1 - c)
        slot = jnp.where(part == 0, 1 - t, t)
        return pltpu.make_async_remote_copy(
            src_ref=oall.at[src, h], dst_ref=orecv.at[slot, h], send_sem=os_sem.at[part, h], recv_sem=or_sem.at[part, h],
            device_id=to_c, device_id_type=MESH)

    for h in range(HC):
        o_lo = attend(h, lo0, 128)
        o_hi = attend(h, hi0, 256)
        oall[0, h] = o_lo[:32]
        oall[1, h] = o_lo[32:]
        oall[3, h] = o_hi[:32]
        oall[2, h] = o_hi[32:]
        for part in range(2):
            o_copy(h, part).start()
    for h in range(HC):
        oown[1 - t, h] = oall[c, h]
        oown[t, h] = oall[2 + c, h]
    for h in range(HC):
        for part in range(2):
            o_copy(h, part).wait_recv()

    wo_copy().wait()
    mine = pl.multiple_of(c * 1024, 1024)
    other = pl.multiple_of((1 - c) * 1024, 1024)

    def y_copy(n):
        return pltpu.make_async_remote_copy(
            src_ref=ysend.at[n], dst_ref=yrecv.at[n], send_sem=ys_sem.at[n], recv_sem=yr_sem.at[n],
            device_id=to_y, device_id_type=MESH)

    def out_proj(n, _):
        cols = pl.ds(pl.multiple_of(n * NB, NB), NB)
        acc = jnp.zeros((64, NB), F32)
        for h in range(HC):
            a = jnp.concatenate([oown[0, h], oown[1, h]], axis=0)
            acc += jnp.dot(a, wo[pl.ds(mine + h * E, E), cols], preferred_element_type=F32)
        for h in range(HC):
            a = jnp.concatenate([orecv[0, h], orecv[1, h]], axis=0)
            acc += jnp.dot(a, wo[pl.ds(other + h * E, E), cols], preferred_element_type=F32)
        ysend[n] = acc[:32]
        yown[n] = acc[32:]
        y_copy(n).start()
        return 0

    lax.fori_loop(0, NN, out_proj, 0)

    for n in range(NN):
        y_copy(n).wait_recv()
        out_ref[:, n * NB:(n + 1) * NB] = (yown[n] + yrecv[n]).astype(BF16)

    for k in range(NK):
        for kind in range(7):
            send(kind, k, own, to_y).wait_send()
    for h in range(HC):
        for part in range(2):
            o_copy(h, part).wait_send()
    for n in range(NN):
        y_copy(n).wait_send()


def solution(mesh):
    def device_fn(x_loc, w_q, w_k, w_v, w_o):
        def view(w):
            w = w.reshape(NK, 2, 256, 2, HC, 2, 128)
            return w.transpose(0, 1, 2, 5, 3, 4, 6)

        any_spec = pl.BlockSpec(memory_space=pl.ANY)
        dma = pltpu.SemaphoreType.DMA
        return pl.pallas_call(
            kernel,
            out_shape=jax.ShapeDtypeStruct((ROWS, D), BF16),
            in_specs=[any_spec] * 5,
            out_specs=pl.BlockSpec(memory_space=pltpu.VMEM),
            scratch_shapes=[
                pltpu.VMEM((SEQ, D), BF16),
                pltpu.VMEM((3, NK, 256, 2, 8, 128), BF16),
                pltpu.VMEM((3 * HC, D, E), BF16),
                pltpu.VMEM((2 * HC * E, D), BF16),
                pltpu.VMEM((3 * HC, SEQ, E), BF16),
                pltpu.VMEM((4, HC, 32, E), BF16),
                pltpu.VMEM((2, HC, 32, E), BF16),
                pltpu.VMEM((2, HC, 32, E), BF16),
                pltpu.VMEM((NN, 32, NB), F32),
                pltpu.VMEM((NN, 32, NB), F32),
                pltpu.VMEM((NN, 32, NB), F32),
                dma, dma((3, NK, 2)), dma,
                dma((7, NK)), dma((7, NK)),
                dma((2, HC)), dma((2, HC)),
                dma((NN,)), dma((NN,)),
            ],
            compiler_params=pltpu.CompilerParams(
                collective_id=0, has_side_effects=True, vmem_limit_bytes=63 << 20),
            name="mha",
        )(x_loc, view(w_q), view(w_k), view(w_v), w_o.reshape(2 * HC * E, D))

    seq_spec = P(("dp", "cp", "tp"), None)
    head_spec = P(None, "tp", None)
    return jax.shard_map(device_fn, mesh=mesh, in_specs=(seq_spec, head_spec, head_spec, head_spec, P("tp", None, None)), out_specs=seq_spec, check_vma=False)
```

```python
import functools

import jax
import jax.numpy as jnp
from jax import lax
from jax.experimental import pallas as pl
from jax.experimental.pallas import tpu as pltpu
from jax.sharding import PartitionSpec as P

MESH = pl.DeviceIdType.MESH
BF16 = jnp.bfloat16
F32 = jnp.float32

ROWS = 32
SEQ = 256
D = 3072
E = 256
HC = 4
KB = 512
NK = D // KB
DH = D // 2
NB = 256
NN = D // NB
NEG = -1e30
OWN_Y, OWN_X, OWN_C, FWD, Y_C, X_C, G_C = range(7)


def kernel(x_hbm, wq_hbm, wk_hbm, wv_hbm, wo_hbm, out_ref,
           xg, raw, wd, wo, xq, qb, kvacc, kv, oall, oown, orecv, yown, ysend, yrecv,
           x_sem, w_sem, wo_sem, xs_sem, xr_sem, os_sem, or_sem, ys_sem, yr_sem):
    t = lax.axis_index("tp")
    cp = lax.axis_index("cp")
    xx = cp // 2
    c = cp % 2
    cx = (cp + 2) % 4
    to_y = {"tp": 1 - t}
    to_x = {"cp": cx}
    to_c = {"cp": cp + 1 - 2 * c}

    def block(tt, pp):
        return pp + tt * (7 - 2 * pp)

    own = block(t, cp)
    b_y = block(1 - t, cp)
    b_x = block(t, cx)
    b_g = block(1 - t, cx)

    def x_rows(b, k):
        return xg.at[pl.ds(pl.multiple_of(b * ROWS, ROWS), ROWS), pl.ds(pl.multiple_of(k * KB, KB), KB)]

    x_copy = pltpu.make_async_copy(x_hbm, xg.at[pl.ds(pl.multiple_of(own * ROWS, ROWS), ROWS), :], x_sem)
    x_copy.start()

    def w_copy(m, k, half):
        src = (wq_hbm, wk_hbm, wv_hbm)[m]
        return pltpu.make_async_copy(src.at[k, half, :, :, c], raw.at[m, k, :, :, pl.ds(4 * half, 4)], w_sem.at[m, k, half])

    def wo_copy():
        return pltpu.make_async_copy(wo_hbm, wo, wo_sem)

    barrier = pltpu.get_barrier_semaphore()
    for peer in (to_y, to_x, to_c):
        pl.semaphore_signal(barrier, inc=1, device_id=peer, device_id_type=MESH)
    with jax.named_scope("xwait"):
        x_copy.wait()
    for k in range(NK):
        for m in range(3):
            for half in range(2):
                w_copy(m, k, half).start()
    wo_copy().start()
    with jax.named_scope("barrier"):
        pl.semaphore_wait(barrier, 3)

    def send(kind, k, b, peer):
        return pltpu.make_async_remote_copy(
            src_ref=x_rows(b, k), dst_ref=x_rows(b, k), send_sem=xs_sem.at[kind, k], recv_sem=xr_sem.at[kind, k],
            device_id=peer, device_id_type=MESH)

    for k in range(NK):
        send(OWN_Y, k, own, to_y).start()
        send(OWN_X, k, own, to_x).start()
    for k in range(NK):
        send(OWN_C, k, own, to_c).start()

    def handle_direct(k):
        send(OWN_Y, k, b_y, to_y).wait_recv()
        even = k % 2 == 0
        send(Y_C, k, b_y, to_c).start()
        if even:
            send(FWD, k, b_y, to_x).start()
        send(OWN_X, k, b_x, to_x).wait_recv()
        send(X_C, k, b_x, to_c).start()
        if not even:
            send(FWD, k, b_x, to_y).start()

    def handle_diag(k):
        send(FWD, k, b_g, to_x).wait_recv()
        send(G_C, k, b_g, to_c).start()

    def deint(m, k):
        for half in range(2):
            w_copy(m, k, half).wait()
        for j in range(2):
            for q in range(4):
                v = jnp.swapaxes(raw[m, k, pl.ds(q * 64, 64), j], 0, 1)
                for half in range(2):
                    for h in range(HC):
                        wd[m * HC + h, pl.ds(k * KB + half * 256 + q * 64, 64), pl.ds(j * 128, 128)] = v[half * 4 + h]

    lo0 = pl.multiple_of(xx * 64, 64)
    hi0 = pl.multiple_of(192 - xx * 64, 64)
    p_own = block(t, cp + 1 - 2 * c)
    p_y = block(1 - t, cp + 1 - 2 * c)
    p_cp = (cp + 1 - 2 * c + 2) % 4
    p_x = block(t, p_cp)
    p_g = block(1 - t, p_cp)

    for k in range(NK):
        with jax.named_scope(f"deint{k}"):
            for m in range(3):
                deint(m, k)
        if k >= 2:
            with jax.named_scope(f"direct{k - 2}"):
                handle_direct(k - 2)
    for k in range(NK - 2, NK):
        with jax.named_scope(f"direct{k}"):
            handle_direct(k)
    with jax.named_scope("qwait"):
        for k in range(NK):
            send(OWN_C, k, p_own, to_c).wait_recv()
            send(Y_C, k, p_y, to_c).wait_recv()
    xq[:64] = xg[pl.ds(lo0, 64), :]
    xq[64:] = xg[pl.ds(hi0, 64), :]
    for h in range(2):
        with jax.named_scope(f"qproj{h}"):
            for i in (2 * h, 2 * h + 1):
                qb[i] = jnp.dot(xq[...], wd[i], preferred_element_type=F32).astype(BF16)
        with jax.named_scope(f"diag{h}"):
            for k in range(3 * h, 3 * h + 3):
                handle_diag(k)

    with jax.named_scope("kvwait0"):
        for k in range(3):
            send(X_C, k, p_x, to_c).wait_recv()
            send(G_C, k, p_g, to_c).wait_recv()

    def kv_first(i, _):
        kvacc[i] = jnp.dot(xg[:, :DH], wd[HC + i, :DH], preferred_element_type=F32)
        return 0

    with jax.named_scope("kv0"):
        lax.fori_loop(0, 2 * HC, kv_first, 0, unroll=4)
    with jax.named_scope("kvwait1"):
        for k in range(3, NK):
            send(X_C, k, p_x, to_c).wait_recv()
            send(G_C, k, p_g, to_c).wait_recv()

    def kv_second(i, _):
        kv[i] = (kvacc[i] + jnp.dot(xg[:, DH:], wd[HC + i, DH:], preferred_element_type=F32)).astype(BF16)
        return 0

    with jax.named_scope("kv1"):
        lax.fori_loop(0, 2 * HC, kv_second, 0, unroll=4)

    def attend(part, start, n_keys):
        heads = range(HC)
        rows = start + lax.broadcasted_iota(jnp.int32, (64, n_keys), 0)
        seen = lax.broadcasted_iota(jnp.int32, (64, n_keys), 1) <= rows
        s = [lax.dot_general(qb[h, part * 64:part * 64 + 64, :], kv[h, :n_keys, :], (((1,), (1,)), ((), ())), preferred_element_type=F32)
             for h in heads]
        s = [jnp.where(seen, v * (E ** -0.5), NEG) for v in s]
        m = [jnp.max(v, axis=-1, keepdims=True) for v in s]
        p = [jnp.exp(v - w) for v, w in zip(s, m)]
        l = [jnp.sum(v, axis=-1, keepdims=True) for v in p]
        o = [jnp.dot(p[h].astype(BF16), kv[HC + h, :n_keys, :], preferred_element_type=F32) for h in heads]
        return [(o[h] / l[h]).astype(BF16) for h in heads]

    def o_copy(h, part):
        src = 2 * part + (1 - c)
        slot = jnp.where(part == 0, 1 - t, t)
        return pltpu.make_async_remote_copy(
            src_ref=oall.at[src, h], dst_ref=orecv.at[slot, h], send_sem=os_sem.at[part, h], recv_sem=or_sem.at[part, h],
            device_id=to_c, device_id_type=MESH)

    with jax.named_scope("attn"):
        o_lo = attend(0, lo0, 128)
        o_hi = attend(1, hi0, 256)
        for h in range(HC):
            oall[0, h] = o_lo[h][:32]
            oall[1, h] = o_lo[h][32:]
            oall[3, h] = o_hi[h][:32]
            oall[2, h] = o_hi[h][32:]
    for h in range(HC):
        for part in range(2):
            o_copy(h, part).start()
    for h in range(HC):
        oown[1 - t, h] = oall[c, h]
        oown[t, h] = oall[2 + c, h]
    with jax.named_scope("owait"):
        for h in range(HC):
            for part in range(2):
                o_copy(h, part).wait_recv()
    with jax.named_scope("wowait"):
        wo_copy().wait()
    mine = pl.multiple_of(c * 1024, 1024)
    other = pl.multiple_of((1 - c) * 1024, 1024)

    def y_copy(n):
        return pltpu.make_async_remote_copy(
            src_ref=ysend.at[n], dst_ref=yrecv.at[n], send_sem=ys_sem.at[n], recv_sem=yr_sem.at[n],
            device_id=to_y, device_id_type=MESH)

    def out_proj(n, _):
        cols = pl.ds(pl.multiple_of(n * NB, NB), NB)
        acc = jnp.zeros((64, NB), F32)
        for h in range(HC):
            a = jnp.concatenate([oown[0, h], oown[1, h]], axis=0)
            acc += jnp.dot(a, wo[pl.ds(mine + h * E, E), cols], preferred_element_type=F32)
        for h in range(HC):
            a = jnp.concatenate([orecv[0, h], orecv[1, h]], axis=0)
            acc += jnp.dot(a, wo[pl.ds(other + h * E, E), cols], preferred_element_type=F32)
        ysend[n] = acc[:32]
        yown[n] = acc[32:]
        y_copy(n).start()
        return 0

    with jax.named_scope('outproj'):
        lax.fori_loop(0, NN, out_proj, 0)

    for n in range(NN):
        with jax.named_scope(f"yw{n}"):
            y_copy(n).wait_recv()
        out_ref[:, n * NB:(n + 1) * NB] = (yown[n] + yrecv[n]).astype(BF16)

    for k in range(NK):
        for kind in range(7):
            send(kind, k, own, to_y).wait_send()
    for h in range(HC):
        for part in range(2):
            o_copy(h, part).wait_send()
    for n in range(NN):
        y_copy(n).wait_send()


def solution(mesh):
    def device_fn(x_loc, w_q, w_k, w_v, w_o):
        def view(w):
            w = w.reshape(NK, 2, 256, 2, HC, 2, 128)
            return w.transpose(0, 1, 2, 5, 3, 4, 6)

        any_spec = pl.BlockSpec(memory_space=pl.ANY)
        dma = pltpu.SemaphoreType.DMA
        return pl.pallas_call(
            kernel,
            out_shape=pltpu.VMEM((ROWS, D), BF16),
            in_specs=[any_spec] * 5,
            out_specs=pl.BlockSpec(memory_space=pltpu.VMEM),
            scratch_shapes=[
                pltpu.VMEM((SEQ, D), BF16),
                pltpu.VMEM((3, NK, 256, 2, 8, 128), BF16),
                pltpu.VMEM((3 * HC, D, E), BF16),
                pltpu.VMEM((2 * HC * E, D), BF16),
                pltpu.VMEM((128, D), BF16),
                pltpu.VMEM((HC, 128, E), BF16),
                pltpu.VMEM((2 * HC, SEQ, E), F32),
                pltpu.VMEM((2 * HC, SEQ, E), BF16),
                pltpu.VMEM((4, HC, 32, E), BF16),
                pltpu.VMEM((2, HC, 32, E), BF16),
                pltpu.VMEM((2, HC, 32, E), BF16),
                pltpu.VMEM((NN, 32, NB), F32),
                pltpu.VMEM((NN, 32, NB), F32),
                pltpu.VMEM((NN, 32, NB), F32),
                dma, dma((3, NK, 2)), dma,
                dma((7, NK)), dma((7, NK)),
                dma((2, HC)), dma((2, HC)),
                dma((NN,)), dma((NN,)),
            ],
            compiler_params=pltpu.CompilerParams(
                collective_id=0, has_side_effects=True, vmem_limit_bytes=63 << 20),
            name="mha",
        )(x_loc, view(w_q), view(w_k), view(w_v), w_o.reshape(2 * HC * E, D))

    seq_spec = P(("dp", "cp", "tp"), None)
    head_spec = P(None, "tp", None)
    return jax.shard_map(device_fn, mesh=mesh, in_specs=(seq_spec, head_spec, head_spec, head_spec, P("tp", None, None)), out_specs=seq_spec, check_vma=False)
```

```python
import functools

import jax
import jax.numpy as jnp
from jax import lax
from jax.experimental import pallas as pl
from jax.experimental.pallas import tpu as pltpu
from jax.sharding import PartitionSpec as P

MESH = pl.DeviceIdType.MESH
BF16 = jnp.bfloat16
F32 = jnp.float32

ROWS = 32
SEQ = 256
D = 3072
E = 256
HC = 4
KB = 512
NK = D // KB
NB = 256
NN = D // NB
NEG = -1e30
OWN_Y, OWN_X, OWN_C, FWD, Y_C, X_C, G_C = range(7)


def kernel(x_hbm, wq_hbm, wk_hbm, wv_hbm, wo_hbm, out_ref,
           xg, raw, wd, wo, qacc, qb, kvacc, kv, oall, oown, orecv, yown, ysend, yrecv,
           x_sem, w_sem, wo_sem, xs_sem, xr_sem, os_sem, or_sem, ys_sem, yr_sem):
    t = lax.axis_index("tp")
    cp = lax.axis_index("cp")
    xx = cp // 2
    c = cp % 2
    cx = (cp + 2) % 4
    to_y = {"tp": 1 - t}
    to_x = {"cp": cx}
    to_c = {"cp": cp + 1 - 2 * c}

    def block(tt, pp):
        return pp + tt * (7 - 2 * pp)

    own = block(t, cp)
    b_y = block(1 - t, cp)
    b_x = block(t, cx)
    b_g = block(1 - t, cx)

    def x_rows(b, k):
        return xg.at[pl.ds(pl.multiple_of(b * ROWS, ROWS), ROWS), pl.ds(pl.multiple_of(k * KB, KB), KB)]

    x_copy = pltpu.make_async_copy(x_hbm, xg.at[pl.ds(pl.multiple_of(own * ROWS, ROWS), ROWS), :], x_sem)
    x_copy.start()

    def w_copy(m, k, half):
        src = (wq_hbm, wk_hbm, wv_hbm)[m]
        return pltpu.make_async_copy(src.at[k, half, :, :, c], raw.at[m, k, :, :, pl.ds(4 * half, 4)], w_sem.at[3 * k + m if k < 2 else 4 + k])

    def wo_copy():
        return pltpu.make_async_copy(wo_hbm, wo, wo_sem)

    barrier = pltpu.get_barrier_semaphore()
    for peer in (to_y, to_x, to_c):
        pl.semaphore_signal(barrier, inc=1, device_id=peer, device_id_type=MESH)
    with jax.named_scope("xwait"):
        x_copy.wait()
    for k in range(NK):
        for m in range(3):
            for half in range(2):
                w_copy(m, k, half).start()
    wo_copy().start()
    with jax.named_scope("barrier"):
        pl.semaphore_wait(barrier, 3)

    def group(kind, k):
        return {OWN_Y: k, OWN_X: k, FWD: 6 + k // 2, OWN_C: 9 + k // 2, Y_C: 9 + k // 2, X_C: 12 + k // 2, G_C: 12 + k // 2}[kind]

    def send(kind, k, b, peer):
        pltpu.make_async_remote_copy(
            src_ref=x_rows(b, k), dst_ref=x_rows(b, k), send_sem=xs_sem, recv_sem=xr_sem.at[group(kind, k)],
            device_id=peer, device_id_type=MESH).start()

    def arrived(kind, k, pieces):
        whole = xg.at[:ROWS * pieces, :KB]
        pltpu.make_async_remote_copy(
            src_ref=whole, dst_ref=whole, send_sem=xs_sem, recv_sem=xr_sem.at[group(kind, k)],
            device_id=to_c, device_id_type=MESH).wait_recv()

    for k in range(NK):
        send(OWN_Y, k, own, to_y)
        send(OWN_X, k, own, to_x)
    for k in range(NK):
        send(OWN_C, k, own, to_c)

    def handle_direct(k):
        with jax.named_scope(f"direct{k}"):
            arrived(OWN_Y, k, 2)
            if k % 2 == 0:
                send(FWD, k, b_y, to_x)
            else:
                send(FWD, k, b_x, to_y)
            send(Y_C, k, b_y, to_c)
            send(X_C, k, b_x, to_c)

    def handle_diag(k):
        with jax.named_scope(f"diag{k}"):
            arrived(FWD, k, 2)
            send(G_C, k, b_g, to_c)
            send(G_C, k + 1, b_g, to_c)

    def weights_here(m, k):
        if k < 2:
            pltpu.make_async_copy(raw.at[m, k], raw.at[m, k], w_sem.at[3 * k + m]).wait()
        elif m == 0:
            pltpu.make_async_copy(raw.at[:, k], raw.at[:, k], w_sem.at[4 + k]).wait()

    def deint(m, k, piece):
        j, q = piece // 4, piece % 4
        v = jnp.swapaxes(raw[m, k, pl.ds(q * 64, 64), j], 0, 1)
        for half in range(2):
            for h in range(HC):
                wd[m * HC + h, pl.ds(k * KB + half * 256 + q * 64, 64), pl.ds(j * 128, 128)] = v[half * 4 + h]

    lo0 = pl.multiple_of(xx * 64, 64)
    hi0 = pl.multiple_of(192 - xx * 64, 64)

    def q_part(part, h):
        cols = slice(part * 2 * KB, (part + 1) * 2 * KB)
        xq = jnp.concatenate([xg[pl.ds(lo0, 64), cols], xg[pl.ds(hi0, 64), cols]], axis=0)
        q = jnp.dot(xq, wd[h, cols], preferred_element_type=F32)
        if part > 0:
            q = qacc[h] + q
        if part < 2:
            qacc[h] = q
        else:
            qb[h] = q.astype(BF16)

    def step(name, weights, part=None):
        with jax.named_scope(name):
            for m, k in weights:
                weights_here(m, k)
            if part is not None:
                arrived(OWN_C, 2 * part, 4)
            pieces = [(m, k, piece) for m, k in weights for piece in range(8)]
            dots = list(range(HC)) if part is not None else []
            for i, (m, k, piece) in enumerate(pieces):
                if dots and i * HC >= len(pieces) * (HC - len(dots)):
                    q_part(part, dots.pop(0))
                deint(m, k, piece)
            for h in dots:
                q_part(part, h)

    for k in range(2):
        for m in range(3):
            step(f"s{k}{m}", [(m, k)])
    step("s20", [(0, 2)])
    handle_direct(0)
    step("s21", [(1, 2), (2, 2)])
    handle_direct(1)
    step("s30", [(0, 3), (1, 3)])
    handle_direct(2)
    step("s32", [(2, 3), (0, 4)])
    handle_direct(3)
    step("s41", [(1, 4), (2, 4)], 0)
    handle_direct(4)
    step("s50", [(0, 5), (1, 5)])
    handle_direct(5)
    step("s52", [(2, 5)], 1)
    handle_diag(0)
    step("q2", [], 2)
    handle_diag(2)

    for part in range(3):
        cols = slice(part * 2 * KB, (part + 1) * 2 * KB)
        with jax.named_scope(f"kvwait{part}"):
            arrived(X_C, 2 * part, 4)

        def kv_part(i, _, part=part, cols=cols):
            y = jnp.dot(xg[:, cols], wd[HC + i, cols], preferred_element_type=F32)
            if part > 0:
                y = kvacc[i] + y
            if part < 2:
                kvacc[i] = y
            else:
                kv[i] = y.astype(BF16)
            return 0

        with jax.named_scope(f"kv{part}"):
            lax.fori_loop(0, 2 * HC, kv_part, 0, unroll=True)
        if part == 0:
            handle_diag(4)

    def attend(part, start, n_keys):
        heads = range(HC)
        rows = start + lax.broadcasted_iota(jnp.int32, (64, n_keys), 0)
        seen = lax.broadcasted_iota(jnp.int32, (64, n_keys), 1) <= rows
        s = [lax.dot_general(qb[h, part * 64:part * 64 + 64, :], kv[h, :n_keys, :], (((1,), (1,)), ((), ())), preferred_element_type=F32)
             for h in heads]
        s = [jnp.where(seen, v * (E ** -0.5), NEG) for v in s]
        m = [jnp.max(v, axis=-1, keepdims=True) for v in s]
        p = [jnp.exp(v - w) for v, w in zip(s, m)]
        l = [jnp.sum(v, axis=-1, keepdims=True) for v in p]
        o = [jnp.dot(p[h].astype(BF16), kv[HC + h, :n_keys, :], preferred_element_type=F32) for h in heads]
        return [(o[h] / l[h]).astype(BF16) for h in heads]

    def o_send(part):
        src = 2 * part + (1 - c)
        slot = 1 - t if part == 0 else t
        pltpu.make_async_remote_copy(
            src_ref=oall.at[src], dst_ref=orecv.at[slot], send_sem=os_sem, recv_sem=or_sem,
            device_id=to_c, device_id_type=MESH).start()

    def o_all():
        return pltpu.make_async_remote_copy(
            src_ref=orecv, dst_ref=orecv, send_sem=os_sem, recv_sem=or_sem, device_id=to_c, device_id_type=MESH)

    with jax.named_scope("attn"):
        o_lo = attend(0, lo0, 128)
        o_hi = attend(1, hi0, 256)
        for h in range(HC):
            oall[0, h] = o_lo[h][:32]
            oall[1, h] = o_lo[h][32:]
            oall[3, h] = o_hi[h][:32]
            oall[2, h] = o_hi[h][32:]
    for part in range(2):
        o_send(part)
    for h in range(HC):
        oown[1 - t, h] = oall[c, h]
        oown[t, h] = oall[2 + c, h]
    with jax.named_scope("owait"):
        o_all().wait_recv()
    with jax.named_scope("wowait"):
        wo_copy().wait()
    mine = pl.multiple_of(c * 1024, 1024)
    other = pl.multiple_of((1 - c) * 1024, 1024)

    def y_send(n):
        pltpu.make_async_remote_copy(
            src_ref=ysend.at[n], dst_ref=yrecv.at[n], send_sem=ys_sem, recv_sem=yr_sem.at[n // 6 + n // 9 + n // 11],
            device_id=to_y, device_id_type=MESH).start()

    def y_arrived(i, first, last):
        some = yrecv.at[first:last]
        pltpu.make_async_remote_copy(
            src_ref=some, dst_ref=some, send_sem=ys_sem, recv_sem=yr_sem.at[i], device_id=to_y, device_id_type=MESH).wait_recv()

    def out_proj(n, _):
        cols = pl.ds(pl.multiple_of(n * NB, NB), NB)
        acc = jnp.zeros((64, NB), F32)
        for h in range(HC):
            a = jnp.concatenate([oown[0, h], oown[1, h]], axis=0)
            acc += jnp.dot(a, wo[pl.ds(mine + h * E, E), cols], preferred_element_type=F32)
        for h in range(HC):
            a = jnp.concatenate([orecv[0, h], orecv[1, h]], axis=0)
            acc += jnp.dot(a, wo[pl.ds(other + h * E, E), cols], preferred_element_type=F32)
        ysend[n] = acc[:32]
        yown[n] = acc[32:]
        y_send(n)
        return 0

    with jax.named_scope('outproj'):
        lax.fori_loop(0, NN, out_proj, 0)

    for i, (first, last) in enumerate(((0, 6), (6, 9), (9, 11), (11, 12))):
        with jax.named_scope(f"yw{i}"):
            y_arrived(i, first, last)
        for n in range(first, last):
            out_ref[:, n * NB:(n + 1) * NB] = (yown[n] + yrecv[n]).astype(BF16)

    sent = xg.at[:7 * ROWS]
    pltpu.make_async_remote_copy(
        src_ref=sent, dst_ref=sent, send_sem=xs_sem, recv_sem=xr_sem.at[0], device_id=to_c, device_id_type=MESH).wait_send()
    o_all().wait_send()
    pltpu.make_async_remote_copy(
        src_ref=ysend, dst_ref=ysend, send_sem=ys_sem, recv_sem=yr_sem.at[0], device_id=to_y, device_id_type=MESH).wait_send()


def solution(mesh):
    def device_fn(x_loc, w_q, w_k, w_v, w_o):
        def view(w):
            w = w.reshape(NK, 2, 256, 2, HC, 2, 128)
            return w.transpose(0, 1, 2, 5, 3, 4, 6)

        any_spec = pl.BlockSpec(memory_space=pl.ANY)
        dma = pltpu.SemaphoreType.DMA
        return pl.pallas_call(
            kernel,
            out_shape=pltpu.VMEM((ROWS, D), BF16),
            in_specs=[any_spec] * 5,
            out_specs=pl.BlockSpec(memory_space=pltpu.VMEM),
            scratch_shapes=[
                pltpu.VMEM((SEQ, D), BF16),
                pltpu.VMEM((3, NK, 256, 2, 8, 128), BF16),
                pltpu.VMEM((3 * HC, D, E), BF16),
                pltpu.VMEM((2 * HC * E, D), BF16),
                pltpu.VMEM((HC, 128, E), F32),
                pltpu.VMEM((HC, 128, E), BF16),
                pltpu.VMEM((2 * HC, SEQ, E), F32),
                pltpu.VMEM((2 * HC, SEQ, E), BF16),
                pltpu.VMEM((4, HC, 32, E), BF16),
                pltpu.VMEM((2, HC, 32, E), BF16),
                pltpu.VMEM((2, HC, 32, E), BF16),
                pltpu.VMEM((NN, 32, NB), F32),
                pltpu.VMEM((NN, 32, NB), F32),
                pltpu.VMEM((NN, 32, NB), F32),
                dma, dma((10,)), dma,
                dma, dma((15,)),
                dma, dma,
                dma, dma((4,)),
            ],
            compiler_params=pltpu.CompilerParams(
                collective_id=0, has_side_effects=True, vmem_limit_bytes=63 << 20),
            name="mha",
        )(x_loc, view(w_q), view(w_k), view(w_v), w_o.reshape(2 * HC * E, D))

    seq_spec = P(("dp", "cp", "tp"), None)
    head_spec = P(None, "tp", None)
    return jax.shard_map(device_fn, mesh=mesh, in_specs=(seq_spec, head_spec, head_spec, head_spec, P("tp", None, None)), out_specs=seq_spec, check_vma=False)
```

```python
import functools

import jax
import jax.numpy as jnp
from jax import lax
from jax.experimental import pallas as pl
from jax.experimental.pallas import tpu as pltpu
from jax.sharding import PartitionSpec as P

MESH = pl.DeviceIdType.MESH
BF16 = jnp.bfloat16
F32 = jnp.float32

ROWS = 32
SEQ = 256
D = 3072
E = 256
HC = 4
KB = 512
NK = D // KB
NB = 256
NN = D // NB
NEG = -1e30
YO = (0, 2, 4, 1, 3, 5)
XO = (1, 3, 5, 0, 2, 4)
OWN_Y, OWN_X, OWN_C, FWD, Y_C, X_C, G_C = range(7)


def kernel(x_hbm, wq_hbm, wk_hbm, wv_hbm, wo_hbm, out_ref,
           xg, raw, wd, wo, qacc, qb, kvacc, kv, oall, orecv, yown, ysend, yrecv,
           x_sem, w_sem, wo_sem, xs_sem, xr_sem, os_sem, or_sem, ys_sem, yr_sem):
    t = lax.axis_index("tp")
    cp = lax.axis_index("cp")
    xx = cp // 2
    c = cp % 2
    pc = cp + 1 - 2 * c
    to_c = {"cp": pc}
    to_y = {"tp": 1 - t, "cp": pc}
    to_x = {"cp": (pc + 2) % 4}

    def block(tt, pp):
        return pp + tt * (7 - 2 * pp)

    own = block(t, cp)
    b_y = block(1 - t, pc)
    b_x = block(t, (pc + 2) % 4)
    b_g = block(1 - t, (cp + 2) % 4)

    def x_rows(b, k):
        return xg.at[pl.ds(pl.multiple_of(b * ROWS, ROWS), ROWS), pl.ds(pl.multiple_of(k * KB, KB), KB)]

    x_copy = pltpu.make_async_copy(x_hbm, xg.at[pl.ds(pl.multiple_of(own * ROWS, ROWS), ROWS), :], x_sem)
    x_copy.start()

    def w_copy(m, k, half):
        src = (wq_hbm, wk_hbm, wv_hbm)[m]
        return pltpu.make_async_copy(src.at[k, half, :, :, c], raw.at[m, k, :, :, pl.ds(4 * half, 4)], w_sem.at[3 * k + m])

    def wo_copy():
        return pltpu.make_async_copy(wo_hbm, wo, wo_sem)

    barrier = pltpu.get_barrier_semaphore()
    for peer in (to_y, to_x, to_c):
        pl.semaphore_signal(barrier, inc=1, device_id=peer, device_id_type=MESH)
    with jax.named_scope("xwait"):
        x_copy.wait()
    for k in range(NK):
        for m in range(3):
            for half in range(2):
                w_copy(m, k, half).start()
    with jax.named_scope("barrier"):
        pl.semaphore_wait(barrier, 3)

    def group(kind, k):
        at = {OWN_Y: YO.index(k), OWN_X: XO.index(k), FWD: 6 + k // 2, X_C: 12 + k // 2, G_C: 12 + k // 2}
        return at.get(kind, 9 + YO.index(k) // 2)

    def send(kind, k, b, peer):
        pltpu.make_async_remote_copy(
            src_ref=x_rows(b, k), dst_ref=x_rows(b, k), send_sem=xs_sem, recv_sem=xr_sem.at[group(kind, k)],
            device_id=peer, device_id_type=MESH).start()

    def arrived(kind, k, pieces):
        whole = xg.at[:ROWS * pieces, :KB]
        pltpu.make_async_remote_copy(
            src_ref=whole, dst_ref=whole, send_sem=xs_sem, recv_sem=xr_sem.at[group(kind, k)],
            device_id=to_c, device_id_type=MESH).wait_recv()

    for i in range(NK):
        send(OWN_Y, YO[i], own, to_y)
        send(OWN_X, XO[i], own, to_x)
    for i in range(NK):
        send(OWN_C, YO[i], own, to_c)

    def handle_direct(i):
        with jax.named_scope(f"direct{i}"):
            arrived(OWN_Y, YO[i], 2)
            if i < 3:
                send(FWD, YO[i], b_y, to_x)
                send(FWD, XO[i], b_x, to_y)
            send(Y_C, YO[i], b_y, to_c)
            send(X_C, XO[i], b_x, to_c)

    def handle_diag(k):
        with jax.named_scope(f"diag{k}"):
            arrived(FWD, k, 2)
            send(G_C, k, b_g, to_c)
            send(G_C, k + 1, b_g, to_c)

    def weights_here(m, k):
        pltpu.make_async_copy(raw.at[m, k], raw.at[m, k], w_sem.at[3 * k + m]).wait()

    def deint(m, k, piece):
        j, q = piece // 4, piece % 4
        v = jnp.swapaxes(raw[m, k, pl.ds(q * 64, 64), j], 0, 1)
        for half in range(2):
            for h in range(HC):
                wd[m * HC + h, pl.ds(k * KB + half * 256 + q * 64, 64), pl.ds(j * 128, 128)] = v[half * 4 + h]

    lo0 = pl.multiple_of(xx * 64, 64)
    hi0 = pl.multiple_of(192 - xx * 64, 64)

    def q_part(part, h):
        q = None
        for k in YO[2 * part:2 * part + 2]:
            cols = slice(k * KB, (k + 1) * KB)
            xq = jnp.concatenate([xg[pl.ds(lo0, 64), cols], xg[pl.ds(hi0, 64), cols]], axis=0)
            z = jnp.dot(xq, wd[h, cols], preferred_element_type=F32)
            q = z if q is None else q + z
        if part > 0:
            q = qacc[h] + q
        if part < 2:
            qacc[h] = q
        else:
            qb[h] = q.astype(BF16)

    def step(name, weights, part=None):
        with jax.named_scope(name):
            for m, k in weights:
                weights_here(m, k)
            if part is not None:
                arrived(OWN_C, YO[2 * part], 4)
            pieces = [(m, k, piece) for m, k in weights for piece in range(8)]
            dots = list(range(HC)) if part is not None else []
            for i, (m, k, piece) in enumerate(pieces):
                if dots and i * HC >= len(pieces) * (HC - len(dots)):
                    q_part(part, dots.pop(0))
                deint(m, k, piece)
            for h in dots:
                q_part(part, h)

    def steps(first, last):
        for i in range(first, last):
            step(f"s{i // 3}{i % 3}", [(i % 3, i // 3)])

    first_chip = jnp.logical_and(t == 0, xx == 0)

    def schedule(marks):
        done = 0
        for i, mark in enumerate(marks):
            steps(done, mark)
            done = mark
            if mark == 18 and i == NK - 1:
                step("q0", [], 0)
            handle_direct(i)
        if done < 18:
            steps(done, 18)
            step("q0", [], 0)

    @pl.when(first_chip)
    def _():
        schedule((10, 12, 14, 16, 18, 18))

    @pl.when(jnp.logical_not(first_chip))
    def _():
        schedule((7, 9, 11, 13, 15, 17))

    handle_diag(0)
    step("q1", [], 1)
    handle_diag(2)
    step("q2", [], 2)

    def kv_part(part):
        cols = slice(part * 2 * KB, (part + 1) * 2 * KB)
        with jax.named_scope(f"kvwait{part}"):
            arrived(X_C, 2 * part, 4)
        with jax.named_scope(f"kv{part}"):
            for i in range(2 * HC):
                y = jnp.dot(xg[:, cols], wd[HC + i, cols], preferred_element_type=F32)
                if part > 0:
                    y = kvacc[i] + y
                if part < 2:
                    kvacc[i] = y
                else:
                    kv[i] = y.astype(BF16)

    wo_copy().start()
    kv_part(0)
    handle_diag(4)
    kv_part(1)
    kv_part(2)

    def attend(part):
        start = pl.multiple_of(lo0 + part * (hi0 - lo0), 64)
        heads = range(HC)
        rows = start + lax.broadcasted_iota(jnp.int32, (64, SEQ), 0)
        seen = lax.broadcasted_iota(jnp.int32, (64, SEQ), 1) <= rows
        s = [lax.dot_general(qb[h, pl.ds(pl.multiple_of(part * 64, 64), 64), :], kv[h], (((1,), (1,)), ((), ())),
                             preferred_element_type=F32) for h in heads]
        s = [jnp.where(seen, v * (E ** -0.5), NEG) for v in s]
        m = [jnp.max(v, axis=-1, keepdims=True) for v in s]
        p = [jnp.exp(v - w) for v, w in zip(s, m)]
        l = [jnp.sum(v, axis=-1, keepdims=True) for v in p]
        o = [jnp.dot(p[h].astype(BF16), kv[HC + h], preferred_element_type=F32) for h in heads]
        for h in heads:
            z = (o[h] / l[h]).astype(BF16)
            oall[2 * part, h] = z[:32]
            oall[2 * part + 1, h] = z[32:]

    def o_rows(part, core):
        return oall.at[2 * part + (core + part - 2 * core * part)]

    def core_of(core, slot):
        return 1 - core if slot == 0 else core

    def o_send(part, slot):
        pltpu.make_async_remote_copy(
            src_ref=o_rows(part, core_of(1 - c, slot)), dst_ref=orecv.at[slot], send_sem=os_sem, recv_sem=or_sem.at[slot],
            device_id=to_c, device_id_type=MESH).start()

    def o_arrived(slot):
        pltpu.make_async_remote_copy(
            src_ref=orecv.at[slot], dst_ref=orecv.at[slot], send_sem=os_sem, recv_sem=or_sem.at[slot],
            device_id=to_c, device_id_type=MESH).wait_recv()

    parts = (1 - t, t)
    mine = pl.multiple_of(c * 1024, 1024)
    other = pl.multiple_of((1 - c) * 1024, 1024)

    def y_part(slot, n):
        cols = pl.ds(pl.multiple_of(n * NB, NB), NB)
        acc = jnp.zeros((ROWS, NB), F32)
        for h in range(HC):
            acc += jnp.dot(o_rows(parts[slot], core_of(c, slot))[h], wo[pl.ds(mine + h * E, E), cols], preferred_element_type=F32)
        for h in range(HC):
            acc += jnp.dot(orecv[slot, h], wo[pl.ds(other + h * E, E), cols], preferred_element_type=F32)
        return acc

    def y_send(n):
        pltpu.make_async_remote_copy(
            src_ref=ysend.at[n], dst_ref=yrecv.at[n], send_sem=ys_sem, recv_sem=yr_sem.at[n // 6 + n // 9 + n // 11],
            device_id=to_y, device_id_type=MESH).start()

    def y_arrived(i, first, last):
        some = yrecv.at[first:last]
        pltpu.make_async_remote_copy(
            src_ref=some, dst_ref=some, send_sem=ys_sem, recv_sem=yr_sem.at[i], device_id=to_y, device_id_type=MESH).wait_recv()

    with jax.named_scope("attn0"):
        attend(parts[0])
    o_send(parts[0], 0)
    with jax.named_scope("attn1"):
        attend(parts[1])
    o_send(parts[1], 1)
    with jax.named_scope("wowait"):
        wo_copy().wait()
    with jax.named_scope("owait0"):
        o_arrived(0)

    def out_peer(n, _):
        ysend[n] = y_part(0, n)
        y_send(n)
        return 0

    with jax.named_scope("outproj0"):
        lax.fori_loop(0, NN, out_peer, 0)
    with jax.named_scope("owait1"):
        o_arrived(1)

    def out_own(n, _):
        yown[n] = y_part(1, n)
        return 0

    with jax.named_scope("outproj1"):
        lax.fori_loop(0, NN, out_own, 0)

    for i, (first, last) in enumerate(((0, 6), (6, 9), (9, 11), (11, 12))):
        with jax.named_scope(f"yw{i}"):
            y_arrived(i, first, last)
        for n in range(first, last):
            out_ref[:, n * NB:(n + 1) * NB] = (yown[n] + yrecv[n]).astype(BF16)

    sent = xg.at[:7 * ROWS]
    pltpu.make_async_remote_copy(
        src_ref=sent, dst_ref=sent, send_sem=xs_sem, recv_sem=xr_sem.at[0], device_id=to_c, device_id_type=MESH).wait_send()
    pltpu.make_async_remote_copy(
        src_ref=orecv, dst_ref=orecv, send_sem=os_sem, recv_sem=or_sem.at[0], device_id=to_c, device_id_type=MESH).wait_send()
    pltpu.make_async_remote_copy(
        src_ref=ysend, dst_ref=ysend, send_sem=ys_sem, recv_sem=yr_sem.at[0], device_id=to_y, device_id_type=MESH).wait_send()


def solution(mesh):
    def device_fn(x_loc, w_q, w_k, w_v, w_o):
        def view(w):
            w = w.reshape(NK, 2, 256, 2, HC, 2, 128)
            return w.transpose(0, 1, 2, 5, 3, 4, 6)

        any_spec = pl.BlockSpec(memory_space=pl.ANY)
        dma = pltpu.SemaphoreType.DMA
        return pl.pallas_call(
            kernel,
            out_shape=pltpu.VMEM((ROWS, D), BF16),
            in_specs=[any_spec] * 5,
            out_specs=pl.BlockSpec(memory_space=pltpu.VMEM),
            scratch_shapes=[
                pltpu.VMEM((SEQ, D), BF16),
                pltpu.VMEM((3, NK, 256, 2, 8, 128), BF16),
                pltpu.VMEM((3 * HC, D, E), BF16),
                pltpu.VMEM((2 * HC * E, D), BF16),
                pltpu.VMEM((HC, 128, E), F32),
                pltpu.VMEM((HC, 128, E), BF16),
                pltpu.VMEM((2 * HC, SEQ, E), F32),
                pltpu.VMEM((2 * HC, SEQ, E), BF16),
                pltpu.VMEM((4, HC, 32, E), BF16),
                pltpu.VMEM((2, HC, 32, E), BF16),
                pltpu.VMEM((NN, 32, NB), F32),
                pltpu.VMEM((NN, 32, NB), F32),
                pltpu.VMEM((NN, 32, NB), F32),
                dma, dma((18,)), dma,
                dma, dma((15,)),
                dma, dma((2,)),
                dma, dma((4,)),
            ],
            compiler_params=pltpu.CompilerParams(
                collective_id=0, has_side_effects=True, vmem_limit_bytes=63 << 20),
            name="mha",
        )(x_loc, view(w_q), view(w_k), view(w_v), w_o.reshape(2 * HC * E, D))

    seq_spec = P(("dp", "cp", "tp"), None)
    head_spec = P(None, "tp", None)
    return jax.shard_map(device_fn, mesh=mesh, in_specs=(seq_spec, head_spec, head_spec, head_spec, P("tp", None, None)), out_specs=seq_spec, check_vma=False)
```

```python
import functools

import jax
import jax.numpy as jnp
from jax import lax
from jax.experimental import pallas as pl
from jax.experimental.pallas import tpu as pltpu
from jax.sharding import PartitionSpec as P

MESH = pl.DeviceIdType.MESH
BF16 = jnp.bfloat16
F32 = jnp.float32

ROWS = 32
SEQ = 256
D = 3072
E = 256
HC = 4
KB = 512
NK = D // KB
NB = 256
NN = D // NB
NEG = -1e30
RR = 2
YO = (0, 2, 4, 1, 3, 5)
XO = (1, 3, 5, 0, 2, 4)
OWN_Y, OWN_X, OWN_C, FWD, Y_C, X_C, G_C = range(7)


def kernel(x_hbm, wq_hbm, wk_hbm, wv_hbm, wo_hbm, out_ref,
           xg, raw, wd, wo, qacc, qb, kvacc, kv, oall, orecv, yown, ysend, yrecv, yfwd,
           w_sem, xs_sem, xr_sem, os_sem, or_sem, ys_sem, yr_sem, yf_sem):
    t = lax.axis_index("tp")
    cp = lax.axis_index("cp")
    xx = cp // 2
    c = cp % 2
    pc = cp + 1 - 2 * c
    to_c = {"cp": pc}
    to_y = {"tp": 1 - t, "cp": pc}
    to_x = {"cp": (pc + 2) % 4}

    def block(tt, pp):
        return pp + tt * (7 - 2 * pp)

    own = block(t, cp)
    b_y = block(1 - t, pc)
    b_x = block(t, (pc + 2) % 4)
    b_g = block(1 - t, (cp + 2) % 4)

    def x_rows(b, k):
        return xg.at[pl.ds(pl.multiple_of(b * ROWS, ROWS), ROWS), pl.ds(pl.multiple_of(k * KB, KB), KB)]

    def x_copy(k):
        return pltpu.make_async_copy(x_hbm.at[:, pl.ds(k * KB, KB)], x_rows(own, k), w_sem.at[k])

    for k in range(NK):
        x_copy(k).start()

    def w_copy(m, k, half):
        src = (wq_hbm, wk_hbm, wv_hbm)[m]
        return pltpu.make_async_copy(src.at[k, half, :, :, c], raw.at[m, k, :, :, pl.ds(4 * half, 4)], w_sem.at[3 * k + m])

    def wo_copy():
        return pltpu.make_async_copy(wo_hbm, wo, w_sem.at[0])

    barrier = pltpu.get_barrier_semaphore()
    for peer in (to_y, to_x, to_c):
        pl.semaphore_signal(barrier, inc=1, device_id=peer, device_id_type=MESH)
    with jax.named_scope("xwait"):
        for k in range(NK):
            x_copy(k).wait()
    for k in range(NK):
        for m in range(3):
            for half in range(2):
                w_copy(m, k, half).start()
    with jax.named_scope("barrier"):
        pl.semaphore_wait(barrier, 3)

    def group(kind, k):
        at = {OWN_Y: YO.index(k), OWN_X: XO.index(k), FWD: 6 + k // 2, X_C: 12 + k // 2, G_C: 12 + k // 2}
        return at.get(kind, 9 + YO.index(k) // 2)

    def send(kind, k, b, peer):
        pltpu.make_async_remote_copy(
            src_ref=x_rows(b, k), dst_ref=x_rows(b, k), send_sem=xs_sem, recv_sem=xr_sem.at[group(kind, k)],
            device_id=peer, device_id_type=MESH).start()

    def arrived(kind, k, pieces):
        whole = xg.at[:ROWS * pieces, :KB]
        pltpu.make_async_remote_copy(
            src_ref=whole, dst_ref=whole, send_sem=xs_sem, recv_sem=xr_sem.at[group(kind, k)],
            device_id=to_c, device_id_type=MESH).wait_recv()

    for i in range(NK):
        send(OWN_Y, YO[i], own, to_y)
        send(OWN_X, XO[i], own, to_x)
    for i in range(NK):
        send(OWN_C, YO[i], own, to_c)

    def handle_direct(i):
        with jax.named_scope(f"direct{i}"):
            arrived(OWN_Y, YO[i], 2)
            if i < 3:
                send(FWD, YO[i], b_y, to_x)
                send(FWD, XO[i], b_x, to_y)
            send(Y_C, YO[i], b_y, to_c)
            send(X_C, XO[i], b_x, to_c)

    def handle_diag(k):
        with jax.named_scope(f"diag{k}"):
            arrived(FWD, k, 2)
            send(G_C, k, b_g, to_c)
            send(G_C, k + 1, b_g, to_c)

    def weights_here(m, k):
        pltpu.make_async_copy(raw.at[m, k], raw.at[m, k], w_sem.at[3 * k + m]).wait()

    def deint(m, k, piece):
        j, q = piece // 4, piece % 4
        v = jnp.swapaxes(raw[m, k, pl.ds(q * 64, 64), j], 0, 1)
        for half in range(2):
            for h in range(HC):
                wd[m * HC + h, pl.ds(k * KB + half * 256 + q * 64, 64), pl.ds(j * 128, 128)] = v[half * 4 + h]

    lo0 = pl.multiple_of(xx * 64, 64)
    hi0 = pl.multiple_of(192 - xx * 64, 64)

    def q_part(part, h):
        q = None
        for k in YO[2 * part:2 * part + 2]:
            cols = slice(k * KB, (k + 1) * KB)
            xq = jnp.concatenate([xg[pl.ds(lo0, 64), cols], xg[pl.ds(hi0, 64), cols]], axis=0)
            z = jnp.dot(xq, wd[h, cols], preferred_element_type=F32)
            q = z if q is None else q + z
        if part > 0:
            q = qacc[h] + q
        if part < 2:
            qacc[h] = q
        else:
            qb[h] = q.astype(BF16)

    def step(name, weights, part=None):
        with jax.named_scope(name):
            for m, k in weights:
                weights_here(m, k)
            if part is not None:
                arrived(OWN_C, YO[2 * part], 4)
            pieces = [(m, k, piece) for m, k in weights for piece in range(8)]
            dots = list(range(HC)) if part is not None else []
            for i, (m, k, piece) in enumerate(pieces):
                if dots and i * HC >= len(pieces) * (HC - len(dots)):
                    q_part(part, dots.pop(0))
                deint(m, k, piece)
            for h in dots:
                q_part(part, h)

    def steps(first, last):
        for i in range(first, last):
            step(f"s{i // 3}{i % 3}", [(i % 3, i // 3)])

    first_chip = jnp.logical_and(t == 0, xx == 0)

    def schedule(marks):
        done = 0
        for i, mark in enumerate(marks):
            steps(done, mark)
            done = mark
            if mark == 18 and i == NK - 1:
                step("q0", [], 0)
            handle_direct(i)
        if done < 18:
            steps(done, 18)
            step("q0", [], 0)

    @pl.when(first_chip)
    def _():
        schedule((10, 12, 14, 16, 18, 18))

    @pl.when(jnp.logical_not(first_chip))
    def _():
        schedule((7, 9, 11, 13, 15, 17))

    handle_diag(0)
    step("q1", [], 1)
    handle_diag(2)
    step("q2", [], 2)

    def kv_part(part):
        cols = slice(part * 2 * KB, (part + 1) * 2 * KB)
        with jax.named_scope(f"kvwait{part}"):
            arrived(X_C, 2 * part, 4)
        with jax.named_scope(f"kv{part}"):
            for i in range(2 * HC):
                y = jnp.dot(xg[:, cols], wd[HC + i, cols], preferred_element_type=F32)
                if part > 0:
                    y = kvacc[i] + y
                if part < 2:
                    kvacc[i] = y
                else:
                    kv[i] = y.astype(BF16)

    wo_copy().start()
    kv_part(0)
    handle_diag(4)
    kv_part(1)
    kv_part(2)

    def attend(part):
        start = pl.multiple_of(lo0 + part * (hi0 - lo0), 64)
        heads = range(HC)
        rows = start + lax.broadcasted_iota(jnp.int32, (64, SEQ), 0)
        seen = lax.broadcasted_iota(jnp.int32, (64, SEQ), 1) <= rows
        s = [lax.dot_general(qb[h, pl.ds(pl.multiple_of(part * 64, 64), 64), :], kv[h], (((1,), (1,)), ((), ())),
                             preferred_element_type=F32) for h in heads]
        s = [jnp.where(seen, v * (E ** -0.5), NEG) for v in s]
        m = [jnp.max(v, axis=-1, keepdims=True) for v in s]
        p = [jnp.exp(v - w) for v, w in zip(s, m)]
        l = [jnp.sum(v, axis=-1, keepdims=True) for v in p]
        o = [jnp.dot(p[h].astype(BF16), kv[HC + h], preferred_element_type=F32) for h in heads]
        for h in heads:
            z = (o[h] / l[h]).astype(BF16)
            oall[2 * part, h] = z[:32]
            oall[2 * part + 1, h] = z[32:]

    def o_rows(part, core):
        return oall.at[2 * part + (core + part - 2 * core * part)]

    def core_of(core, slot):
        return 1 - core if slot == 0 else core

    def o_send(part, slot):
        pltpu.make_async_remote_copy(
            src_ref=o_rows(part, core_of(1 - c, slot)), dst_ref=orecv.at[slot], send_sem=os_sem, recv_sem=or_sem.at[slot],
            device_id=to_c, device_id_type=MESH).start()

    def o_arrived(slot):
        pltpu.make_async_remote_copy(
            src_ref=orecv.at[slot], dst_ref=orecv.at[slot], send_sem=os_sem, recv_sem=or_sem.at[slot],
            device_id=to_c, device_id_type=MESH).wait_recv()

    parts = (1 - t, t)
    mine = pl.multiple_of(c * 1024, 1024)
    other = pl.multiple_of((1 - c) * 1024, 1024)

    def y_half(slot, n, far):
        cols = pl.ds(pl.multiple_of(n * NB, NB), NB)
        acc = jnp.zeros((ROWS, NB), F32)
        for h in range(HC):
            if far:
                acc += jnp.dot(orecv[slot, h], wo[pl.ds(other + h * E, E), cols], preferred_element_type=F32)
            else:
                acc += jnp.dot(o_rows(parts[slot], core_of(c, slot))[h], wo[pl.ds(mine + h * E, E), cols], preferred_element_type=F32)
        return acc

    def y_part(slot, n):
        return y_half(slot, n, False) + y_half(slot, n, True)

    def from_chip(n):
        return jnp.logical_and(jnp.logical_and(t == 1, xx == 0), c <= 1 - n)

    def by_chip(n):
        return jnp.logical_and(jnp.logical_and(t == 0, xx == 1), c <= 1 - n)

    def y_round(n):
        return pltpu.make_async_remote_copy(
            src_ref=ysend.at[n], dst_ref=yfwd.at[n], send_sem=ys_sem, recv_sem=yf_sem.at[n],
            device_id={"tp": 1 - t, "cp": (cp + 2) % 4}, device_id_type=MESH)

    def y_forward(n):
        return pltpu.make_async_remote_copy(
            src_ref=yfwd.at[n], dst_ref=yrecv.at[n], send_sem=yf_sem.at[RR + n], recv_sem=yr_sem.at[4 + n],
            device_id=to_x, device_id_type=MESH)

    def y_first(n):
        @pl.when(from_chip(n))
        def _():
            y_round(n).start()

        @pl.when(jnp.logical_not(from_chip(n)))
        def _():
            pltpu.make_async_remote_copy(
                src_ref=ysend.at[n], dst_ref=yrecv.at[n], send_sem=ys_sem, recv_sem=yr_sem.at[4 + n],
                device_id=to_y, device_id_type=MESH).start()

    def y_send(n):
        pltpu.make_async_remote_copy(
            src_ref=ysend.at[n], dst_ref=yrecv.at[n], send_sem=ys_sem, recv_sem=yr_sem.at[n // 6 + n // 9 + n // 11],
            device_id=to_y, device_id_type=MESH).start()

    def y_arrived(i, first, last):
        some = yrecv.at[first:last]
        pltpu.make_async_remote_copy(
            src_ref=some, dst_ref=some, send_sem=ys_sem, recv_sem=yr_sem.at[i], device_id=to_y, device_id_type=MESH).wait_recv()

    with jax.named_scope("attn0"):
        attend(parts[0])
    o_send(parts[0], 0)
    with jax.named_scope("attn1"):
        attend(parts[1])
    o_send(parts[1], 1)
    with jax.named_scope("wowait"):
        wo_copy().wait()
    with jax.named_scope("early"):
        yown[0] = y_half(0, RR, False)
    with jax.named_scope("owait0"):
        o_arrived(0)

    def out_peer(n, _):
        ysend[n] = y_part(0, n)
        y_send(n)
        return 0

    with jax.named_scope("outproj0"):
        ysend[RR] = yown[0] + y_half(0, RR, True)
        y_send(RR)
        for n in range(RR):
            ysend[n] = y_part(0, n)
            y_first(n)
        lax.fori_loop(RR + 1, NN, out_peer, 0)
    with jax.named_scope("forward"):
        for n in range(RR):
            @pl.when(by_chip(n))
            def _(n=n):
                y_round(n).wait_recv()
                y_forward(n).start()
    with jax.named_scope("owait1"):
        o_arrived(1)

    def out_own(n, _):
        yown[n] = y_part(1, n)
        return 0

    with jax.named_scope("outproj1"):
        lax.fori_loop(0, NN, out_own, 0)

    for i, (first, last) in enumerate(((RR, 6), (6, 9), (9, 11), (11, 12))):
        with jax.named_scope(f"yw{i}"):
            y_arrived(i, first, last)
        if i == 2:
            for n in range(RR):
                y_arrived(4 + n, n, n + 1)
        for n in range(first if i != 2 else 0, last):
            if i == 2 and RR <= n < first:
                continue
            out_ref[:, n * NB:(n + 1) * NB] = (yown[n] + yrecv[n]).astype(BF16)

    sent = xg.at[:7 * ROWS]
    pltpu.make_async_remote_copy(
        src_ref=sent, dst_ref=sent, send_sem=xs_sem, recv_sem=xr_sem.at[0], device_id=to_c, device_id_type=MESH).wait_send()
    pltpu.make_async_remote_copy(
        src_ref=orecv, dst_ref=orecv, send_sem=os_sem, recv_sem=or_sem.at[0], device_id=to_c, device_id_type=MESH).wait_send()
    pltpu.make_async_remote_copy(
        src_ref=ysend, dst_ref=ysend, send_sem=ys_sem, recv_sem=yr_sem.at[0], device_id=to_y, device_id_type=MESH).wait_send()

    for n in range(RR):
        @pl.when(by_chip(n))
        def _(n=n):
            y_forward(n).wait_send()


def solution(mesh):
    def device_fn(x_loc, w_q, w_k, w_v, w_o):
        def view(w):
            w = w.reshape(NK, 2, 256, 2, HC, 2, 128)
            return w.transpose(0, 1, 2, 5, 3, 4, 6)

        any_spec = pl.BlockSpec(memory_space=pl.ANY)
        dma = pltpu.SemaphoreType.DMA
        return pl.pallas_call(
            kernel,
            out_shape=pltpu.VMEM((ROWS, D), BF16),
            in_specs=[any_spec] * 5,
            out_specs=pl.BlockSpec(memory_space=pltpu.VMEM),
            scratch_shapes=[
                pltpu.VMEM((SEQ, D), BF16),
                pltpu.VMEM((3, NK, 256, 2, 8, 128), BF16),
                pltpu.VMEM((3 * HC, D, E), BF16),
                pltpu.VMEM((2 * HC * E, D), BF16),
                pltpu.VMEM((HC, 128, E), F32),
                pltpu.VMEM((HC, 128, E), BF16),
                pltpu.VMEM((2 * HC, SEQ, E), F32),
                pltpu.VMEM((2 * HC, SEQ, E), BF16),
                pltpu.VMEM((4, HC, 32, E), BF16),
                pltpu.VMEM((2, HC, 32, E), BF16),
                pltpu.VMEM((NN, 32, NB), F32),
                pltpu.VMEM((NN, 32, NB), F32),
                pltpu.VMEM((NN, 32, NB), F32),
                pltpu.VMEM((RR, 32, NB), F32),
                dma((18,)),
                dma, dma((15,)),
                dma, dma((2,)),
                dma, dma((4 + RR,)), dma((2 * RR,)),
            ],
            compiler_params=pltpu.CompilerParams(
                collective_id=0, has_side_effects=True, vmem_limit_bytes=63 << 20),
            name="mha",
        )(x_loc, view(w_q), view(w_k), view(w_v), w_o.reshape(2 * HC * E, D))

    seq_spec = P(("dp", "cp", "tp"), None)
    head_spec = P(None, "tp", None)
    return jax.shard_map(device_fn, mesh=mesh, in_specs=(seq_spec, head_spec, head_spec, head_spec, P("tp", None, None)), out_specs=seq_spec, check_vma=False)
```

```python
import functools

import jax
import jax.numpy as jnp
from jax import lax
from jax.experimental import pallas as pl
from jax.experimental.pallas import tpu as pltpu
from jax.sharding import PartitionSpec as P

MESH = pl.DeviceIdType.MESH
BF16 = jnp.bfloat16
F32 = jnp.float32

ROWS = 32
SEQ = 256
D = 3072
E = 256
HC = 4
KB = 512
NK = D // KB
NB = 256
NN = D // NB
NEG = -1e30
RR = 2
YO = (0, 2, 4, 1, 3, 5)
XO = (1, 3, 5, 0, 2, 4)
OWN_Y, OWN_X, OWN_C, FWD, Y_C, X_C, G_C = range(7)


def kernel(x_hbm, wq_hbm, wk_hbm, wv_hbm, wo_hbm, out_ref,
           xg, raw, wd, wo, qacc, qb, kvacc, kv, oall, orecv, yown, ysend, yrecv, yfwd,
           w_sem, xs_sem, xr_sem, os_sem, or_sem, ys_sem, yr_sem, yf_sem):
    t = lax.axis_index("tp")
    cp = lax.axis_index("cp")
    xx = cp // 2
    c = cp % 2
    pc = cp + 1 - 2 * c
    to_c = {"cp": pc}
    to_y = {"tp": 1 - t, "cp": pc}
    to_x = {"cp": (pc + 2) % 4}

    def block(tt, pp):
        return pp + tt * (7 - 2 * pp)

    own = block(t, cp)
    b_y = block(1 - t, pc)
    b_x = block(t, (pc + 2) % 4)
    b_g = block(1 - t, (cp + 2) % 4)

    def x_rows(b, k):
        return xg.at[pl.ds(pl.multiple_of(b * ROWS, ROWS), ROWS), pl.ds(pl.multiple_of(k * KB, KB), KB)]

    def x_copy(k):
        return pltpu.make_async_copy(x_hbm.at[:, pl.ds(k * KB, KB)], x_rows(own, k), w_sem.at[k])

    for k in range(NK):
        x_copy(k).start()

    def w_copy(m, k, half):
        src = (wq_hbm, wk_hbm, wv_hbm)[m]
        return pltpu.make_async_copy(src.at[k, half, :, :, c], raw.at[m, k, :, :, pl.ds(4 * half, 4)], w_sem.at[3 * k + m])

    def wo_copy():
        return pltpu.make_async_copy(wo_hbm, wo, w_sem.at[0])

    barrier = pltpu.get_barrier_semaphore()
    for peer in (to_y, to_x, to_c):
        pl.semaphore_signal(barrier, inc=1, device_id=peer, device_id_type=MESH)
    with jax.named_scope("xwait"):
        for k in range(NK):
            x_copy(k).wait()
    for k in range(NK):
        for m in range(3):
            for half in range(2):
                w_copy(m, k, half).start()
    with jax.named_scope("barrier"):
        pl.semaphore_wait(barrier, 3)

    def group(kind, k):
        at = {OWN_Y: YO.index(k), OWN_X: XO.index(k), FWD: 6 + k // 2, X_C: 12 + k // 2, G_C: 12 + k // 2}
        return at.get(kind, 9 + YO.index(k) // 2)

    def send(kind, k, b, peer):
        pltpu.make_async_remote_copy(
            src_ref=x_rows(b, k), dst_ref=x_rows(b, k), send_sem=xs_sem, recv_sem=xr_sem.at[group(kind, k)],
            device_id=peer, device_id_type=MESH).start()

    def arrived(kind, k, pieces):
        whole = xg.at[:ROWS * pieces, :KB]
        pltpu.make_async_remote_copy(
            src_ref=whole, dst_ref=whole, send_sem=xs_sem, recv_sem=xr_sem.at[group(kind, k)],
            device_id=to_c, device_id_type=MESH).wait_recv()

    for i in range(NK):
        send(OWN_Y, YO[i], own, to_y)
        send(OWN_X, XO[i], own, to_x)
    for i in range(NK):
        send(OWN_C, YO[i], own, to_c)

    def handle_direct(i):
        with jax.named_scope(f"direct{i}"):
            arrived(OWN_Y, YO[i], 2)
            if i < 3:
                send(FWD, YO[i], b_y, to_x)
                send(FWD, XO[i], b_x, to_y)
            send(Y_C, YO[i], b_y, to_c)
            send(X_C, XO[i], b_x, to_c)

    def handle_diag(k):
        with jax.named_scope(f"diag{k}"):
            arrived(FWD, k, 2)
            send(G_C, k, b_g, to_c)
            send(G_C, k + 1, b_g, to_c)

    def weights_here(m, k):
        pltpu.make_async_copy(raw.at[m, k], raw.at[m, k], w_sem.at[3 * k + m]).wait()

    def deint(m, k, piece):
        j, q = piece // 4, piece % 4
        v = jnp.swapaxes(raw[m, k, pl.ds(q * 64, 64), j], 0, 1)
        for half in range(2):
            for h in range(HC):
                wd[m * HC + h, pl.ds(k * KB + half * 256 + q * 64, 64), pl.ds(j * 128, 128)] = v[half * 4 + h]

    lo0 = pl.multiple_of(xx * 64, 64)
    hi0 = pl.multiple_of(192 - xx * 64, 64)

    def q_part(part, h):
        q = None
        for k in YO[2 * part:2 * part + 2]:
            cols = slice(k * KB, (k + 1) * KB)
            xq = jnp.concatenate([xg[pl.ds(lo0, 64), cols], xg[pl.ds(hi0, 64), cols]], axis=0)
            z = jnp.dot(xq, wd[h, cols], preferred_element_type=F32)
            q = z if q is None else q + z
        if part > 0:
            q = qacc[h] + q
        if part < 2:
            qacc[h] = q
        else:
            qb[h] = q.astype(BF16)

    def step(name, weights, part=None):
        with jax.named_scope(name):
            for m, k in weights:
                weights_here(m, k)
            if part is not None:
                arrived(OWN_C, YO[2 * part], 4)
            pieces = [(m, k, piece) for m, k in weights for piece in range(8)]
            dots = list(range(HC)) if part is not None else []
            for i, (m, k, piece) in enumerate(pieces):
                if dots and i * HC >= len(pieces) * (HC - len(dots)):
                    q_part(part, dots.pop(0))
                deint(m, k, piece)
            for h in dots:
                q_part(part, h)

    def steps(first, last):
        for i in range(first, last):
            step(f"s{i // 3}{i % 3}", [(i % 3, i // 3)])

    first_chip = jnp.logical_and(t == 0, xx == 0)

    def schedule(marks):
        done = 0
        for i, mark in enumerate(marks):
            steps(done, mark)
            done = mark
            if mark == 18 and i == NK - 1:
                step("q0", [], 0)
            handle_direct(i)
        if done < 18:
            steps(done, 18)
            step("q0", [], 0)

    @pl.when(first_chip)
    def _():
        schedule((10, 12, 14, 16, 18, 18))
        step("q1", [], 1)
        handle_diag(0)
        step("q2", [], 2)
        handle_diag(2)

    def others(marks):
        schedule(marks)
        handle_diag(0)
        step("q1", [], 1)
        handle_diag(2)
        step("q2", [], 2)

    @pl.when(jnp.logical_and(jnp.logical_not(first_chip), c == 0))
    def _():
        others((7, 9, 11, 13, 15, 17))

    @pl.when(jnp.logical_and(jnp.logical_not(first_chip), c == 1))
    def _():
        others((9, 11, 13, 15, 17, 18))

    def kv_part(part):
        cols = slice(part * 2 * KB, (part + 1) * 2 * KB)
        with jax.named_scope(f"kvwait{part}"):
            arrived(X_C, 2 * part, 4)
        with jax.named_scope(f"kv{part}"):
            for i in range(2 * HC):
                y = jnp.dot(xg[:, cols], wd[HC + i, cols], preferred_element_type=F32)
                if part > 0:
                    y = kvacc[i] + y
                if part < 2:
                    kvacc[i] = y
                else:
                    kv[i] = y.astype(BF16)

    wo_copy().start()
    kv_part(0)
    handle_diag(4)
    kv_part(1)
    kv_part(2)

    def attend(part, n_keys):
        start = lo0 if part == 0 else hi0
        heads = range(HC)
        rows = start + lax.broadcasted_iota(jnp.int32, (64, n_keys), 0)
        seen = lax.broadcasted_iota(jnp.int32, (64, n_keys), 1) <= rows
        s = [lax.dot_general(qb[h, part * 64:part * 64 + 64, :], kv[h, :n_keys, :], (((1,), (1,)), ((), ())),
                             preferred_element_type=F32) for h in heads]
        s = [jnp.where(seen, v * (E ** -0.5), NEG) for v in s]
        m = [jnp.max(v, axis=-1, keepdims=True) for v in s]
        p = [jnp.exp(v - w) for v, w in zip(s, m)]
        l = [jnp.sum(v, axis=-1, keepdims=True) for v in p]
        o = [jnp.dot(p[h].astype(BF16), kv[HC + h, :n_keys, :], preferred_element_type=F32) for h in heads]
        for h in heads:
            z = (o[h] / l[h]).astype(BF16)
            oall[2 * part, h] = z[:32]
            oall[2 * part + 1, h] = z[32:]

    def o_rows(part, core):
        return oall.at[2 * part + (core + part - 2 * core * part)]

    def core_of(core, slot):
        return 1 - core if slot == 0 else core

    def o_send(part, slot):
        pltpu.make_async_remote_copy(
            src_ref=o_rows(part, core_of(1 - c, slot)), dst_ref=orecv.at[slot], send_sem=os_sem, recv_sem=or_sem.at[slot],
            device_id=to_c, device_id_type=MESH).start()

    def o_arrived(slot):
        pltpu.make_async_remote_copy(
            src_ref=orecv.at[slot], dst_ref=orecv.at[slot], send_sem=os_sem, recv_sem=or_sem.at[slot],
            device_id=to_c, device_id_type=MESH).wait_recv()

    parts = (1 - t, t)
    mine = pl.multiple_of(c * 1024, 1024)
    other = pl.multiple_of((1 - c) * 1024, 1024)

    def y_half(slot, n, far):
        cols = pl.ds(pl.multiple_of(n * NB, NB), NB)
        acc = jnp.zeros((ROWS, NB), F32)
        for h in range(HC):
            if far:
                acc += jnp.dot(orecv[slot, h], wo[pl.ds(other + h * E, E), cols], preferred_element_type=F32)
            else:
                acc += jnp.dot(o_rows(parts[slot], core_of(c, slot))[h], wo[pl.ds(mine + h * E, E), cols], preferred_element_type=F32)
        return acc

    def y_part(slot, n):
        return y_half(slot, n, False) + y_half(slot, n, True)

    from_chip = jnp.logical_and(jnp.logical_and(t == 1, xx == 0), c == 1)
    by_chip = jnp.logical_and(jnp.logical_and(t == 0, xx == 1), c == 1)

    def y_round(n):
        return pltpu.make_async_remote_copy(
            src_ref=ysend.at[n], dst_ref=yfwd.at[n], send_sem=ys_sem, recv_sem=yf_sem.at[n],
            device_id={"tp": 1 - t, "cp": (cp + 2) % 4}, device_id_type=MESH)

    def y_forward(n):
        return pltpu.make_async_remote_copy(
            src_ref=yfwd.at[n], dst_ref=yrecv.at[n], send_sem=yf_sem.at[RR + n], recv_sem=yr_sem.at[4 + n],
            device_id=to_x, device_id_type=MESH)

    def y_first(n):
        @pl.when(from_chip)
        def _():
            y_round(n).start()

        @pl.when(jnp.logical_not(from_chip))
        def _():
            pltpu.make_async_remote_copy(
                src_ref=ysend.at[n], dst_ref=yrecv.at[n], send_sem=ys_sem, recv_sem=yr_sem.at[4 + n],
                device_id=to_y, device_id_type=MESH).start()

    def y_send(n):
        pltpu.make_async_remote_copy(
            src_ref=ysend.at[n], dst_ref=yrecv.at[n], send_sem=ys_sem, recv_sem=yr_sem.at[n // 6 + n // 9 + n // 11],
            device_id=to_y, device_id_type=MESH).start()

    def y_arrived(i, first, last):
        some = yrecv.at[first:last]
        pltpu.make_async_remote_copy(
            src_ref=some, dst_ref=some, send_sem=ys_sem, recv_sem=yr_sem.at[i], device_id=to_y, device_id_type=MESH).wait_recv()

    def attend_both(order):
        for slot, part in enumerate(order):
            with jax.named_scope(f"attn{slot}"):
                attend(part, 128 if part == 0 else SEQ)
            o_send(part, slot)

    @pl.when(t == 1)
    def _():
        attend_both((0, 1))

    @pl.when(t == 0)
    def _():
        attend_both((1, 0))

    with jax.named_scope("wowait"):
        wo_copy().wait()
    with jax.named_scope("early"):
        yown[0] = y_half(0, RR, False)
    with jax.named_scope("owait0"):
        o_arrived(0)

    def out_peer(n, _):
        ysend[n] = y_part(0, n)
        y_send(n)
        return 0

    with jax.named_scope("outproj0"):
        ysend[RR] = yown[0] + y_half(0, RR, True)
        y_send(RR)
        for n in range(RR):
            ysend[n] = y_part(0, n)
            y_first(n)
        lax.fori_loop(RR + 1, NN, out_peer, 0)
    with jax.named_scope("forward"):
        for n in range(RR):
            @pl.when(by_chip)
            def _(n=n):
                y_round(n).wait_recv()
                y_forward(n).start()
    with jax.named_scope("owait1"):
        o_arrived(1)

    def out_own(n, _):
        yown[n] = y_part(1, n)
        return 0

    with jax.named_scope("outproj1"):
        lax.fori_loop(0, NN, out_own, 0)

    for i, (first, last) in enumerate(((RR, 6), (6, 9), (9, 11), (11, 12))):
        with jax.named_scope(f"yw{i}"):
            y_arrived(i, first, last)
        if i == 2:
            for n in range(RR):
                y_arrived(4 + n, n, n + 1)
        for n in range(first if i != 2 else 0, last):
            if i == 2 and RR <= n < first:
                continue
            out_ref[:, n * NB:(n + 1) * NB] = (yown[n] + yrecv[n]).astype(BF16)

    sent = xg.at[:7 * ROWS]
    pltpu.make_async_remote_copy(
        src_ref=sent, dst_ref=sent, send_sem=xs_sem, recv_sem=xr_sem.at[0], device_id=to_c, device_id_type=MESH).wait_send()
    pltpu.make_async_remote_copy(
        src_ref=orecv, dst_ref=orecv, send_sem=os_sem, recv_sem=or_sem.at[0], device_id=to_c, device_id_type=MESH).wait_send()
    pltpu.make_async_remote_copy(
        src_ref=ysend, dst_ref=ysend, send_sem=ys_sem, recv_sem=yr_sem.at[0], device_id=to_y, device_id_type=MESH).wait_send()

    for n in range(RR):
        @pl.when(by_chip)
        def _(n=n):
            y_forward(n).wait_send()


def solution(mesh):
    def device_fn(x_loc, w_q, w_k, w_v, w_o):
        def view(w):
            w = w.reshape(NK, 2, 256, 2, HC, 2, 128)
            return w.transpose(0, 1, 2, 5, 3, 4, 6)

        any_spec = pl.BlockSpec(memory_space=pl.ANY)
        dma = pltpu.SemaphoreType.DMA
        return pl.pallas_call(
            kernel,
            out_shape=pltpu.VMEM((ROWS, D), BF16),
            in_specs=[any_spec] * 5,
            out_specs=pl.BlockSpec(memory_space=pltpu.VMEM),
            scratch_shapes=[
                pltpu.VMEM((SEQ, D), BF16),
                pltpu.VMEM((3, NK, 256, 2, 8, 128), BF16),
                pltpu.VMEM((3 * HC, D, E), BF16),
                pltpu.VMEM((2 * HC * E, D), BF16),
                pltpu.VMEM((HC, 128, E), F32),
                pltpu.VMEM((HC, 128, E), BF16),
                pltpu.VMEM((2 * HC, SEQ, E), F32),
                pltpu.VMEM((2 * HC, SEQ, E), BF16),
                pltpu.VMEM((4, HC, 32, E), BF16),
                pltpu.VMEM((2, HC, 32, E), BF16),
                pltpu.VMEM((NN, 32, NB), F32),
                pltpu.VMEM((NN, 32, NB), F32),
                pltpu.VMEM((NN, 32, NB), F32),
                pltpu.VMEM((RR, 32, NB), F32),
                dma((18,)),
                dma, dma((15,)),
                dma, dma((2,)),
                dma, dma((4 + RR,)), dma((2 * RR,)),
            ],
            compiler_params=pltpu.CompilerParams(
                collective_id=0, has_side_effects=True, vmem_limit_bytes=63 << 20),
            name="mha",
        )(x_loc, view(w_q), view(w_k), view(w_v), w_o.reshape(2 * HC * E, D))

    seq_spec = P(("dp", "cp", "tp"), None)
    head_spec = P(None, "tp", None)
    return jax.shard_map(device_fn, mesh=mesh, in_specs=(seq_spec, head_spec, head_spec, head_spec, P("tp", None, None)), out_specs=seq_spec, check_vma=False)
```

```python
import functools

import jax
import jax.numpy as jnp
from jax import lax
from jax.experimental import pallas as pl
from jax.experimental.pallas import tpu as pltpu
from jax.sharding import PartitionSpec as P

MESH = pl.DeviceIdType.MESH
BF16 = jnp.bfloat16
F32 = jnp.float32

ROWS = 32
SEQ = 256
D = 3072
E = 256
HC = 4
KB = 512
NK = D // KB
NB = 256
NN = D // NB
NEG = -1e30
RR = 2
YO = (0, 2, 4, 1, 3, 5)
XO = (1, 3, 5, 0, 2, 4)
OWN_Y, OWN_X, OWN_C, FWD, Y_C, X_C, G_C = range(7)


def kernel(x_hbm, wq_hbm, wk_hbm, wv_hbm, wo_hbm, out_ref,
           xg, raw, wd, wo, qacc, qb, kvacc, kv, oall, orecv, yown, ysend, yrecv, yfwd,
           w_sem, xs_sem, xr_sem, os_sem, or_sem, ys_sem, yr_sem, yf_sem):
    t = lax.axis_index("tp")
    cp = lax.axis_index("cp")
    xx = cp // 2
    c = cp % 2
    pc = cp + 1 - 2 * c
    to_c = {"cp": pc}
    to_y = {"tp": 1 - t, "cp": pc}
    to_x = {"cp": (pc + 2) % 4}

    def block(tt, pp):
        return pp + tt * (7 - 2 * pp)

    own = block(t, cp)
    b_y = block(1 - t, pc)
    b_x = block(t, (pc + 2) % 4)
    b_g = block(1 - t, (cp + 2) % 4)

    def x_rows(b, k):
        return xg.at[pl.ds(pl.multiple_of(b * ROWS, ROWS), ROWS), pl.ds(pl.multiple_of(k * KB, KB), KB)]

    def x_copy(k):
        return pltpu.make_async_copy(x_hbm.at[:, pl.ds(k * KB, KB)], x_rows(own, k), w_sem.at[k])

    for k in range(NK):
        x_copy(k).start()

    def w_copy(m, k, half):
        src = (wq_hbm, wk_hbm, wv_hbm)[m]
        return pltpu.make_async_copy(src.at[k, half, :, :, c], raw.at[m, k, :, :, pl.ds(4 * half, 4)], w_sem.at[3 * k + m])

    def wo_copy():
        return pltpu.make_async_copy(wo_hbm, wo, w_sem.at[0])

    barrier = pltpu.get_barrier_semaphore()
    for peer in (to_y, to_x, to_c):
        pl.semaphore_signal(barrier, inc=1, device_id=peer, device_id_type=MESH)
    with jax.named_scope("xwait"):
        for k in range(NK):
            x_copy(k).wait()
    for k in range(NK):
        for m in range(3):
            for half in range(2):
                w_copy(m, k, half).start()
    with jax.named_scope("barrier"):
        pl.semaphore_wait(barrier, 3)

    def group(kind, k):
        at = {OWN_Y: YO.index(k), OWN_X: XO.index(k), FWD: 6 + k // 2, X_C: 12 + k // 2, G_C: 12 + k // 2}
        return at.get(kind, 9 + YO.index(k) // 2)

    def send(kind, k, b, peer):
        pltpu.make_async_remote_copy(
            src_ref=x_rows(b, k), dst_ref=x_rows(b, k), send_sem=xs_sem, recv_sem=xr_sem.at[group(kind, k)],
            device_id=peer, device_id_type=MESH).start()

    def arrived(kind, k, pieces):
        whole = xg.at[:ROWS * pieces, :KB]
        pltpu.make_async_remote_copy(
            src_ref=whole, dst_ref=whole, send_sem=xs_sem, recv_sem=xr_sem.at[group(kind, k)],
            device_id=to_c, device_id_type=MESH).wait_recv()

    for i in range(NK):
        send(OWN_Y, YO[i], own, to_y)
        send(OWN_X, XO[i], own, to_x)
    for i in range(NK):
        send(OWN_C, YO[i], own, to_c)

    def handle_direct(i):
        with jax.named_scope(f"direct{i}"):
            arrived(OWN_Y, YO[i], 2)
            if i < 3:
                send(FWD, YO[i], b_y, to_x)
                send(FWD, XO[i], b_x, to_y)
            send(Y_C, YO[i], b_y, to_c)
            send(X_C, XO[i], b_x, to_c)

    def handle_diag(k):
        with jax.named_scope(f"diag{k}"):
            arrived(FWD, k, 2)
            send(G_C, k, b_g, to_c)
            send(G_C, k + 1, b_g, to_c)

    def weights_here(m, k):
        pltpu.make_async_copy(raw.at[m, k], raw.at[m, k], w_sem.at[3 * k + m]).wait()

    def deint(m, k, piece):
        j, q = piece // 4, piece % 4
        v = jnp.swapaxes(raw[m, k, pl.ds(q * 64, 64), j], 0, 1)
        for half in range(2):
            for h in range(HC):
                wd[m * HC + h, pl.ds(k * KB + half * 256 + q * 64, 64), pl.ds(j * 128, 128)] = v[half * 4 + h]

    lo0 = pl.multiple_of(xx * 64, 64)
    hi0 = pl.multiple_of(192 - xx * 64, 64)

    def q_part(part, h):
        q = None
        for k in YO[2 * part:2 * part + 2]:
            cols = slice(k * KB, (k + 1) * KB)
            xq = jnp.concatenate([xg[pl.ds(lo0, 64), cols], xg[pl.ds(hi0, 64), cols]], axis=0)
            z = jnp.dot(xq, wd[h, cols], preferred_element_type=F32)
            q = z if q is None else q + z
        if part > 0:
            q = qacc[h] + q
        if part < 2:
            qacc[h] = q
        else:
            qb[h] = q.astype(BF16)

    def step(name, weights, part=None):
        with jax.named_scope(name):
            for m, k in weights:
                weights_here(m, k)
            if part is not None:
                arrived(OWN_C, YO[2 * part], 4)
            pieces = [(m, k, piece) for m, k in weights for piece in range(8)]
            dots = list(range(HC)) if part is not None else []
            for i, (m, k, piece) in enumerate(pieces):
                if dots and i * HC >= len(pieces) * (HC - len(dots)):
                    q_part(part, dots.pop(0))
                deint(m, k, piece)
            for h in dots:
                q_part(part, h)

    def steps(first, last):
        for i in range(first, last):
            step(f"s{i // 3}{i % 3}", [(i % 3, i // 3)])

    first_chip = jnp.logical_and(t == 0, xx == 0)

    def schedule(marks):
        done = 0
        for i, mark in enumerate(marks):
            steps(done, mark)
            done = mark
            if mark == 18 and i == NK - 1:
                step("q0", [], 0)
            handle_direct(i)
        if done < 18:
            steps(done, 18)
            step("q0", [], 0)

    @pl.when(first_chip)
    def _():
        schedule((10, 12, 14, 16, 18, 18))
        wo_copy().start()
        step("q1", [], 1)
        handle_diag(0)
        step("q2", [], 2)
        handle_diag(2)

    def others(marks):
        schedule(marks)
        handle_diag(0)
        wo_copy().start()
        step("q1", [], 1)
        handle_diag(2)
        step("q2", [], 2)

    @pl.when(jnp.logical_and(jnp.logical_not(first_chip), c == 0))
    def _():
        others((7, 9, 11, 13, 15, 17))

    @pl.when(jnp.logical_and(jnp.logical_not(first_chip), c == 1))
    def _():
        others((9, 11, 13, 15, 17, 18))

    def kv_wait(part):
        with jax.named_scope(f"kvwait{part}"):
            arrived(X_C, 2 * part, 4)

    def kv_heads(part, which):
        cols = slice(part * 2 * KB, (part + 1) * 2 * KB)
        for i in which:
            y = jnp.dot(xg[:, cols], wd[HC + i, cols], preferred_element_type=F32)
            if part > 0:
                y = kvacc[i] + y
            if part < 2:
                kvacc[i] = y
            else:
                kv[i] = y.astype(BF16)

    kv_wait(0)
    with jax.named_scope("kv0"):
        kv_heads(0, range(2 * HC))
    handle_diag(4)
    kv_wait(1)
    with jax.named_scope("kv1"):
        kv_heads(1, range(2 * HC))
    kv_wait(2)

    def scores(part, n_keys):
        start = lo0 if part == 0 else hi0
        heads = range(HC)
        rows = start + lax.broadcasted_iota(jnp.int32, (64, n_keys), 0)
        seen = lax.broadcasted_iota(jnp.int32, (64, n_keys), 1) <= rows
        s = [lax.dot_general(qb[h, part * 64:part * 64 + 64, :], kv[h, :n_keys, :], (((1,), (1,)), ((), ())),
                             preferred_element_type=F32) for h in heads]
        s = [jnp.where(seen, v * (E ** -0.5), NEG) for v in s]
        m = [jnp.max(v, axis=-1, keepdims=True) for v in s]
        p = [jnp.exp(v - w) for v, w in zip(s, m)]
        l = [jnp.sum(v, axis=-1, keepdims=True) for v in p]
        return [v.astype(BF16) for v in p], l

    def attend(part, n_keys, p, l):
        heads = range(HC)
        o = [jnp.dot(p[h], kv[HC + h, :n_keys, :], preferred_element_type=F32) for h in heads]
        for h in heads:
            z = (o[h] / l[h]).astype(BF16)
            oall[2 * part, h] = z[:32]
            oall[2 * part + 1, h] = z[32:]

    def o_rows(part, core):
        return oall.at[2 * part + (core + part - 2 * core * part)]

    def core_of(core, slot):
        return 1 - core if slot == 0 else core

    def o_send(part, slot):
        pltpu.make_async_remote_copy(
            src_ref=o_rows(part, core_of(1 - c, slot)), dst_ref=orecv.at[slot], send_sem=os_sem, recv_sem=or_sem.at[slot],
            device_id=to_c, device_id_type=MESH).start()

    def o_arrived(slot):
        pltpu.make_async_remote_copy(
            src_ref=orecv.at[slot], dst_ref=orecv.at[slot], send_sem=os_sem, recv_sem=or_sem.at[slot],
            device_id=to_c, device_id_type=MESH).wait_recv()

    parts = (1 - t, t)
    mine = pl.multiple_of(c * 1024, 1024)
    other = pl.multiple_of((1 - c) * 1024, 1024)

    def y_half(slot, n, far):
        cols = pl.ds(pl.multiple_of(n * NB, NB), NB)
        acc = jnp.zeros((ROWS, NB), F32)
        for h in range(HC):
            if far:
                acc += jnp.dot(orecv[slot, h], wo[pl.ds(other + h * E, E), cols], preferred_element_type=F32)
            else:
                acc += jnp.dot(o_rows(parts[slot], core_of(c, slot))[h], wo[pl.ds(mine + h * E, E), cols], preferred_element_type=F32)
        return acc

    def y_part(slot, n):
        return y_half(slot, n, False) + y_half(slot, n, True)

    from_chip = jnp.logical_and(jnp.logical_and(t == 1, xx == 0), c == 1)
    by_chip = jnp.logical_and(jnp.logical_and(t == 0, xx == 1), c == 1)

    def y_round(n):
        return pltpu.make_async_remote_copy(
            src_ref=ysend.at[n], dst_ref=yfwd.at[n], send_sem=ys_sem, recv_sem=yf_sem.at[n],
            device_id={"tp": 1 - t, "cp": (cp + 2) % 4}, device_id_type=MESH)

    def y_forward(n):
        return pltpu.make_async_remote_copy(
            src_ref=yfwd.at[n], dst_ref=yrecv.at[n], send_sem=yf_sem.at[RR + n], recv_sem=yr_sem.at[4 + n],
            device_id=to_x, device_id_type=MESH)

    def y_first(n):
        @pl.when(from_chip)
        def _():
            y_round(n).start()

        @pl.when(jnp.logical_not(from_chip))
        def _():
            pltpu.make_async_remote_copy(
                src_ref=ysend.at[n], dst_ref=yrecv.at[n], send_sem=ys_sem, recv_sem=yr_sem.at[4 + n],
                device_id=to_y, device_id_type=MESH).start()

    def y_send(n):
        pltpu.make_async_remote_copy(
            src_ref=ysend.at[n], dst_ref=yrecv.at[n], send_sem=ys_sem, recv_sem=yr_sem.at[n // 6 + n // 9 + n // 11],
            device_id=to_y, device_id_type=MESH).start()

    def y_arrived(i, first, last):
        some = yrecv.at[first:last]
        pltpu.make_async_remote_copy(
            src_ref=some, dst_ref=some, send_sem=ys_sem, recv_sem=yr_sem.at[i], device_id=to_y, device_id_type=MESH).wait_recv()

    def attend_both(order):
        for slot, part in enumerate(order):
            n_keys = 128 if part == 0 else SEQ
            with jax.named_scope(f"attn{slot}"):
                if slot == 0:
                    kv_heads(2, range(HC))
                p, l = scores(part, n_keys)
                if slot == 0:
                    kv_heads(2, range(HC, 2 * HC))
                attend(part, n_keys, p, l)
            o_send(part, slot)

    @pl.when(t == 1)
    def _():
        attend_both((0, 1))

    @pl.when(t == 0)
    def _():
        attend_both((1, 0))

    with jax.named_scope("wowait"):
        wo_copy().wait()
    with jax.named_scope("early"):
        yown[0] = y_half(0, RR, False)
    with jax.named_scope("owait0"):
        o_arrived(0)

    def out_peer(n, _):
        ysend[n] = y_part(0, n)
        y_send(n)
        return 0

    with jax.named_scope("outproj0"):
        ysend[RR] = yown[0] + y_half(0, RR, True)
        y_send(RR)
        for n in range(RR):
            ysend[n] = y_part(0, n)
            y_first(n)
        lax.fori_loop(RR + 1, NN, out_peer, 0)
    with jax.named_scope("forward"):
        for n in range(RR):
            @pl.when(by_chip)
            def _(n=n):
                y_round(n).wait_recv()
                y_forward(n).start()
    with jax.named_scope("owait1"):
        o_arrived(1)

    def out_own(n, _):
        yown[n] = y_part(1, n)
        return 0

    with jax.named_scope("outproj1"):
        lax.fori_loop(0, NN, out_own, 0)

    for i, (first, last) in enumerate(((RR, 6), (6, 9), (9, 11), (11, 12))):
        with jax.named_scope(f"yw{i}"):
            y_arrived(i, first, last)
        if i == 2:
            for n in range(RR):
                y_arrived(4 + n, n, n + 1)
        for n in range(first if i != 2 else 0, last):
            if i == 2 and RR <= n < first:
                continue
            out_ref[:, n * NB:(n + 1) * NB] = (yown[n] + yrecv[n]).astype(BF16)

    sent = xg.at[:7 * ROWS]
    pltpu.make_async_remote_copy(
        src_ref=sent, dst_ref=sent, send_sem=xs_sem, recv_sem=xr_sem.at[0], device_id=to_c, device_id_type=MESH).wait_send()
    pltpu.make_async_remote_copy(
        src_ref=orecv, dst_ref=orecv, send_sem=os_sem, recv_sem=or_sem.at[0], device_id=to_c, device_id_type=MESH).wait_send()
    pltpu.make_async_remote_copy(
        src_ref=ysend, dst_ref=ysend, send_sem=ys_sem, recv_sem=yr_sem.at[0], device_id=to_y, device_id_type=MESH).wait_send()

    for n in range(RR):
        @pl.when(by_chip)
        def _(n=n):
            y_forward(n).wait_send()


def solution(mesh):
    def device_fn(x_loc, w_q, w_k, w_v, w_o):
        def view(w):
            w = w.reshape(NK, 2, 256, 2, HC, 2, 128)
            return w.transpose(0, 1, 2, 5, 3, 4, 6)

        any_spec = pl.BlockSpec(memory_space=pl.ANY)
        dma = pltpu.SemaphoreType.DMA
        return pl.pallas_call(
            kernel,
            out_shape=pltpu.VMEM((ROWS, D), BF16),
            in_specs=[any_spec] * 5,
            out_specs=pl.BlockSpec(memory_space=pltpu.VMEM),
            scratch_shapes=[
                pltpu.VMEM((SEQ, D), BF16),
                pltpu.VMEM((3, NK, 256, 2, 8, 128), BF16),
                pltpu.VMEM((3 * HC, D, E), BF16),
                pltpu.VMEM((2 * HC * E, D), BF16),
                pltpu.VMEM((HC, 128, E), F32),
                pltpu.VMEM((HC, 128, E), BF16),
                pltpu.VMEM((2 * HC, SEQ, E), F32),
                pltpu.VMEM((2 * HC, SEQ, E), BF16),
                pltpu.VMEM((4, HC, 32, E), BF16),
                pltpu.VMEM((2, HC, 32, E), BF16),
                pltpu.VMEM((NN, 32, NB), F32),
                pltpu.VMEM((NN, 32, NB), F32),
                pltpu.VMEM((NN, 32, NB), F32),
                pltpu.VMEM((RR, 32, NB), F32),
                dma((18,)),
                dma, dma((15,)),
                dma, dma((2,)),
                dma, dma((4 + RR,)), dma((2 * RR,)),
            ],
            compiler_params=pltpu.CompilerParams(
                collective_id=0, has_side_effects=True, vmem_limit_bytes=63 << 20),
            name="mha",
        )(x_loc, view(w_q), view(w_k), view(w_v), w_o.reshape(2 * HC * E, D))

    seq_spec = P(("dp", "cp", "tp"), None)
    head_spec = P(None, "tp", None)
    return jax.shard_map(device_fn, mesh=mesh, in_specs=(seq_spec, head_spec, head_spec, head_spec, P("tp", None, None)), out_specs=seq_spec, check_vma=False)
```
